32 devices in a mesh: grp: 2 (over x), blk: 16 (over z, y, core).
Axes of the slice: x: 2, y: 2, z: 4, core: 2. Of those that a mesh axis runs over, the one named last changes fastest.
Arguments:
- atoms: bfloat16 [16384, 512], P(('grp', 'blk')), parts along dimension 0, may hold values from -8 to 8
- edge_mask: int32 [32, 5, 512, 512], P(('grp', 'blk')), parts along dimension 0, may hold values from 0 to 1
- norm_gain: float32 [512], replicated, may hold values from 0.25 to 1.75
- w_query: bfloat16 [512, 512], replicated, may hold values from -3 to 3
- w_key: bfloat16 [512, 512], replicated, may hold values from -3 to 3
- w_value: bfloat16 [512, 512], replicated, may hold values from -0.25 to 0.25
- w_out: bfloat16 [512, 512], replicated, may hold values from -0.25 to 0.25
- bn_gain: float32 [512], replicated, may hold values from 0.25 to 1.75
- bn_shift: float32 [512], replicated, may hold values from -3 to 3
- w_up: bfloat16 [512, 1024], replicated, may hold values from -0.25 to 0.25
- w_down: bfloat16 [1024, 512], replicated, may hold values from -0.1875 to 0.1875
Outputs:
- updated: bfloat16 [16384, 512], P(('grp', 'blk')), parts along dimension 0
The draws below stay inside these ranges and needn't reach their ends.
There are 2 independent parts, one for each index of `grp`. The reference program is written for one: setup_inputs(seed, part) draws one part's arguments, and reference() takes and returns one part's arrays. A program takes and returns all parts, laid end to end along the dimension named above; an argument that names none is the same for every part. Nothing has to cross between parts.
All inputs are finite; a program needn't handle non-finite values.
Results may differ from the reference program's by a relative error of at most 0.01.
The reference program's roundings to bfloat16 on the way (of `normed`, `query`, `weight`, `mixed`, `batched` and `hidden`) count: a program that leaves them out, or rounds other values in their place, can miss the bound.
Values may be sent and summed in bfloat16 or wider, within the bound.
A program may use at most 128 MiB of HBM per device.

```python
import jax
import jax.numpy as jnp
from jax import lax

D = 512
HEADS = 8
HEAD_DIM = 64
FF = 1024
REACH = 2
TILE = 512
ATOMS = 8192


def draw_atoms(key, part):
    key_base = jax.random.fold_in(key, 11)
    key_one, key_two, key_three, key_four = jax.random.split(key_base, 4)
    ntiles = ATOMS // TILE
    tile_ids = (jnp.arange(ATOMS) // TILE).astype(jnp.int32)
    tile_index = tile_ids.astype(jnp.float32)
    rising = (1.0 + 2.0 * tile_index / (ntiles - 1))[:, None]
    parity = (1 - 2 * (tile_ids % 2)).astype(jnp.float32)[:, None]
    row_scale = jnp.exp(jax.random.uniform(key_two, (ATOMS, 1), jnp.float32, -0.69, 0.69))
    noise = jnp.clip(jax.random.normal(key_one, (ATOMS, D), jnp.float32), -6.0, 6.0)
    feature_mean = jnp.clip(jax.random.normal(key_three, (1, D), jnp.float32), -3.0, 3.0)
    bulk = noise * row_scale * rising + feature_mean * rising
    alternate = jnp.clip(jax.random.normal(key_four, (1, D), jnp.float32), -3.0, 3.0)
    return (0.1 * (bulk + alternate * parity)).astype(jnp.bfloat16)


def projection_draw(key, salt):
    base = jax.random.normal(jax.random.fold_in(key, salt), (D, D), jnp.float32)
    base = jnp.clip(base, -4.0, 4.0) * D ** (-0.5)
    return base.astype(jnp.bfloat16)


def draw_w_query(key, part):
    return projection_draw(key, 21)


def draw_w_key(key, part):
    return projection_draw(key, 22)


def draw_edge_mask(key, part):
    ntiles = ATOMS // TILE
    widths = 2 * REACH + 1
    key_base = jax.random.fold_in(key, 31)
    key_one, key_two, key_three = jax.random.split(key_base, 3)
    cut_level = jax.random.randint(key_one, (ntiles, widths, 1, 1), 0, 12)
    own_level = jax.random.randint(key_two, (ntiles, widths, 1, 1), 6, 24)
    offset = jnp.arange(widths).reshape(1, widths, 1, 1)
    level = jnp.where(offset == REACH, own_level, cut_level)
    draws = jax.random.randint(key_three, (ntiles, widths, TILE, TILE), 0, 64)
    return (draws < level).astype(jnp.int32)


def centred(key, extent, scale, reach, dtype=jnp.bfloat16):
    values = scale * jax.random.normal(key, extent, jnp.float32)
    return jnp.clip(values, min=-reach, max=reach).astype(dtype)


def setup_inputs(seed: int = 0, part: int = 0) -> dict:
    splits = jax.random.split(jax.random.key(seed), 12)
    part_keys = jax.random.split(jax.random.fold_in(splits[11], part), 12)
    return {
        "atoms": draw_atoms(jax.random.fold_in(jax.random.fold_in(splits[11], part), 71), part),
        "edge_mask": draw_edge_mask(jax.random.fold_in(jax.random.fold_in(splits[11], part), 71), part),
        "norm_gain": jnp.clip(1.0 + 0.15 * jax.random.normal(splits[2], (D,), jnp.float32), 0.25, 1.75),
        "w_query": draw_w_query(jax.random.fold_in(splits[11], 71), part),
        "w_key": draw_w_key(jax.random.fold_in(splits[11], 71), part),
        "w_value": centred(splits[5], (D, D), D ** -0.5, 0.25),
        "w_out": centred(splits[6], (D, D), D ** -0.5, 0.25),
        "bn_gain": jnp.clip(1.0 + 0.15 * jax.random.normal(splits[7], (D,), jnp.float32), 0.25, 1.75),
        "bn_shift": centred(splits[8], (D,), 0.5, 3.0, jnp.float32),
        "w_up": centred(splits[9], (D, FF), D ** -0.5, 0.25),
        "w_down": centred(splits[10], (FF, D), FF ** -0.5, 0.1875),
    }


def reference(atoms, edge_mask, norm_gain, w_query, w_key, w_value, w_out, bn_gain, bn_shift, w_up, w_down):
    ntiles = ATOMS // TILE
    widths = 2 * REACH + 1
    scale = HEAD_DIM ** (-0.5)
    xfull = atoms.astype(jnp.float32)
    normed = (xfull * lax.rsqrt(lax.optimization_barrier(jnp.mean(xfull * xfull, axis=-1, keepdims=True)) + 1e-06) * norm_gain).astype(jnp.bfloat16)
    query = jnp.dot(normed, w_query, preferred_element_type=jnp.float32).astype(jnp.bfloat16)
    keys = jnp.dot(normed, w_key, preferred_element_type=jnp.float32).astype(jnp.bfloat16)
    values = jnp.dot(normed, w_value, preferred_element_type=jnp.float32).astype(jnp.bfloat16)
    q_tiles = query.reshape(ntiles, TILE, HEADS, HEAD_DIM)
    k_tiles = keys.reshape(ntiles, TILE, HEADS, HEAD_DIM)
    v_tiles = values.reshape(ntiles, TILE, HEADS, HEAD_DIM)
    k_near = jnp.stack([jnp.roll(k_tiles, -(o - REACH), axis=0) for o in range(widths)], axis=1).reshape(ntiles, widths * TILE, HEADS, HEAD_DIM)
    v_near = jnp.stack([jnp.roll(v_tiles, -(o - REACH), axis=0) for o in range(widths)], axis=1).reshape(ntiles, widths * TILE, HEADS, HEAD_DIM)
    rows = lax.broadcasted_iota(jnp.int32, (TILE, widths, TILE), 0)
    cols = lax.broadcasted_iota(jnp.int32, (TILE, widths, TILE), 2)
    block = lax.broadcasted_iota(jnp.int32, (TILE, widths, TILE), 1)
    selfmask = ((rows == cols) & (block == REACH)).reshape(TILE, widths * TILE)

    def one_tile(pieces):
        qpart, kpart, vpart, mpart = pieces
        allowed = (jnp.transpose(mpart, (1, 0, 2)).reshape(TILE, widths * TILE) > 0) | selfmask
        score = jnp.einsum('qhd,khd->hqk', qpart.astype(jnp.float32), kpart.astype(jnp.float32)) * scale
        score = jnp.where(allowed[None], score, -1e+30)
        top = lax.optimization_barrier(jnp.max(score, axis=-1, keepdims=True))
        expo = jnp.exp(score - top)
        total = lax.optimization_barrier(jnp.sum(expo, axis=-1))
        weight = expo.astype(jnp.bfloat16)
        summed = jnp.einsum('hqk,khd->qhd', weight.astype(jnp.float32), vpart.astype(jnp.float32))
        return (summed / jnp.transpose(total)[:, :, None]).reshape(TILE, D).astype(jnp.bfloat16)
    mixed = lax.map(one_tile, (q_tiles, k_near, v_near, edge_mask)).reshape(ATOMS, D)
    after = xfull + jnp.dot(mixed, w_out, preferred_element_type=jnp.float32)
    mean = lax.optimization_barrier(jnp.mean(after, axis=0))
    var = lax.optimization_barrier(jnp.mean((after - mean) ** 2, axis=0))
    batched = ((after - mean) * lax.rsqrt(var + 1e-05) * bn_gain + bn_shift).astype(jnp.bfloat16)
    hidden = jax.nn.gelu(jnp.dot(batched, w_up, preferred_element_type=jnp.float32), approximate=True).astype(jnp.bfloat16)
    return (after + jnp.dot(hidden, w_down, preferred_element_type=jnp.float32)).astype(jnp.bfloat16)
```

```python
import functools
import math

import jax
import jax.numpy as jnp
from jax import lax
from jax.experimental import pallas as pl
from jax.experimental.pallas import tpu as pltpu
from jax.sharding import PartitionSpec as P

HEAD_DIM = 64
PAIR = 2 * HEAD_DIM
REACH = 2
CHUNKS = 8
PARTS = 4
SUMS = 16
NEG = -1e30
MESH = pl.DeviceIdType.MESH
OWN, PARTNER, MIRROR, RAIL, CROSS = 0, 1, 2, 3, 4
SCALE = math.log2(math.e) * HEAD_DIM ** (-0.5)


def kernel(
    n,
    atoms_hbm, mask_hbm, ng_hbm, wq_hbm, wk_hbm, wv_hbm, wo_hbm, bg_hbm, bs_hbm, wu_hbm, wd_hbm,
    out_ref,
    slab_ref, mask_ref, ng_ref, wq_ref, wk_ref, wv_ref, wo_ref, bg_ref, bs_ref, wu_ref, wd_ref,
    wvt_ref, qt_ref, kb_ref, vt_ref, bias_ref, m_ref, acc_ref, mixed_ref, after_ref,
    stats_ref, load_sem, mask_sem,
    p_send, m_send, r_send, c_send, recv, s_send, s_recv,
):
    me = lax.axis_index("blk")
    rows, width = after_ref.shape
    heads = width // HEAD_DIM
    group, inside = me // 4, me % 4
    side, core = inside // 2, inside % 2
    partner = group * 4 + side * 2 + (1 - core)
    mirror = group * 4 + (1 - side) * 2 + core
    groups = n // 4
    rail_to = ((group + 1 - 2 * side + groups) % groups) * 4 + side * 2 + core
    same = side == core
    late_one = jnp.where(same, RAIL, CROSS)
    late_two = jnp.where(same, CROSS, RAIL)

    barrier = pltpu.get_barrier_semaphore()

    def greet(d, carry):
        pl.semaphore_signal(
            barrier, inc=1, device_id={"blk": lax.rem(me + d, n)}, device_id_type=MESH
        )
        return carry

    lax.fori_loop(1, n, greet, 0)

    sources = (
        (atoms_hbm, slab_ref.at[OWN]), (ng_hbm, ng_ref), (wq_hbm, wq_ref), (wk_hbm, wk_ref),
        (wv_hbm, wv_ref), (wo_hbm, wo_ref), (bg_hbm, bg_ref), (bs_hbm, bs_ref),
        (wu_hbm, wu_ref), (wd_hbm, wd_ref),
    )
    loads = [
        pltpu.make_async_copy(src, dst, load_sem.at[i]) for i, (src, dst) in enumerate(sources)
    ]
    far = jnp.where(side == 0, 2, -2)
    near = jnp.where(core == 0, 1, -1)
    offsets = [jnp.int32(0), near, far, -far, -near]
    masks = [
        pltpu.make_async_copy(
            mask_hbm.at[0, offsets[i] + REACH], mask_ref.at[i], mask_sem.at[i]
        )
        for i in range(2 * REACH + 1)
    ]
    for i in range(5):
        loads[i].start()
    for mask_load in masks:
        mask_load.start()
    for i in range(5, len(loads)):
        loads[i].start()

    step_rows = rows // CHUNKS

    def chunk(c):
        return pl.ds(c * step_rows, step_rows)

    def copy(source, target, c, sem, device):
        return pltpu.make_async_remote_copy(
            src_ref=slab_ref.at[source, chunk(c)], dst_ref=slab_ref.at[target, chunk(c)],
            send_sem=sem.at[c], recv_sem=recv.at[target, c],
            device_id={"blk": device}, device_id_type=MESH,
        )

    def partner_copy(c):
        return copy(OWN, PARTNER, c, p_send, partner)

    def mirror_copy(c):
        return copy(OWN, MIRROR, c, m_send, mirror)

    def rail_copy(c):
        return copy(MIRROR, RAIL, c, r_send, rail_to)

    def cross_copy(c, source):
        return copy(source, CROSS, c, c_send, partner)

    def got_mirror(c):
        mirror_copy(c).wait_recv()
        rail_copy(c).start()

        @pl.when(same)
        def _():
            cross_copy(c, MIRROR).start()

    def got_rail(c):
        rail_copy(c).wait_recv()

        @pl.when(jnp.logical_not(same))
        def _():
            cross_copy(c, RAIL).start()

    def got_cross(c, when):
        @pl.when(when)
        def _():
            cross_copy(c, RAIL).wait_recv()

    loads[0].wait()
    pl.semaphore_wait(barrier, n - 1)
    for c in range(CHUNKS):
        mirror_copy(c).start()
    for c in range(CHUNKS):
        partner_copy(c).start()

    def normalize(value):
        full = value.astype(jnp.float32)
        return (
            full * lax.rsqrt(jnp.mean(full * full, axis=-1, keepdims=True) + 1e-06) * ng_ref[...]
        ).astype(jnp.bfloat16)

    def set_bias(i):
        @pl.when(i == 0)
        def _():
            masks[0].wait()

        for j in range(1, 2 * REACH + 1):
            @pl.when(i == j)
            def _():
                masks[j].wait()

        for k in range(rows // PAIR):
            span = slice(k * PAIR, (k + 1) * PAIR)
            bias_ref[i, span, :] = jnp.where(mask_ref[i, :, span] > 0, 0.0, NEG).T

    def unit(slot, start, count):
        normed = normalize(slab_ref[slot, pl.ds(start, count), :])
        kb_ref[:count] = jnp.dot(
            normed, wk_ref[...], preferred_element_type=jnp.float32
        ).astype(jnp.bfloat16)
        values = lax.dot_general(
            wvt_ref[...], normed, (((1,), (1,)), ((), ())), preferred_element_type=jnp.float32
        ).astype(jnp.bfloat16)
        for h in range(heads):
            vt_ref[h, :HEAD_DIM, :count] = values[h * HEAD_DIM:(h + 1) * HEAD_DIM]

        def scores(h):
            pair = h // 2
            piece = kb_ref[:count, pair * PAIR:(pair + 1) * PAIR]
            return jnp.dot(
                jnp.concatenate([piece, piece], axis=1), qt_ref[h],
                preferred_element_type=jnp.float32,
            ) + bias_ref[slot, pl.ds(start, count), :]

        def finish(h, score):
            old = m_ref[h]
            new = jnp.maximum(old, jnp.max(score, axis=0, keepdims=True))
            m_ref[h] = new
            weight = jnp.exp2(score - new).astype(jnp.bfloat16)
            result = jnp.dot(vt_ref[h, :, :count], weight, preferred_element_type=jnp.float32)
            acc_ref[h] = acc_ref[h] * jnp.exp2(old - new) + result

        ahead = scores(0)
        for h in range(heads):
            current = ahead
            if h + 1 < heads:
                ahead = scores(h + 1)
            finish(h, current)

    ones = jnp.ones((heads, SUMS, vt_ref.shape[2]), jnp.bfloat16)
    vt_ref[:, HEAD_DIM:, :] = ones
    m_ref[...] = jnp.full(m_ref.shape, NEG, jnp.float32)
    acc_ref[...] = jnp.zeros(acc_ref.shape, jnp.float32)

    loads[1].wait()
    normed = normalize(slab_ref[OWN])
    loads[2].wait()
    wqt = wq_ref[...].T
    query = lax.dot_general(
        wqt, normed, (((1,), (1,)), ((), ())), preferred_element_type=jnp.float32
    ).astype(jnp.bfloat16).astype(jnp.float32) * SCALE
    high = query.astype(jnp.bfloat16)
    low = (query - high.astype(jnp.float32)).astype(jnp.bfloat16)
    zero = jnp.zeros((HEAD_DIM, rows), jnp.bfloat16)
    for h in range(heads):
        span = slice(h * HEAD_DIM, (h + 1) * HEAD_DIM)
        for part, base in ((high, 0), (low, PAIR)):
            here = base + (h % 2) * HEAD_DIM
            there = base + (1 - h % 2) * HEAD_DIM
            qt_ref[h, here:here + HEAD_DIM] = part[span]
            qt_ref[h, there:there + HEAD_DIM] = zero
    loads[4].wait()
    wvt_ref[...] = wv_ref[...].T
    loads[3].wait()
    set_bias(0)
    eye = lax.broadcasted_iota(jnp.int32, (rows, rows), 0) == lax.broadcasted_iota(
        jnp.int32, (rows, rows), 1
    )
    bias_ref[0] = jnp.where(eye, 0.0, bias_ref[0])

    per = CHUNKS // PARTS
    half = rows // 2
    quarter = rows // PARTS

    events = {
        0: (),
        1: (),
        2: (("p", 0, 8),),
        3: (("m", 0, 1),),
        4: (("m", 1, 4), ("r", 0, 1)),
        5: (
            ("m", 4, 5), ("r", 1, 2), ("m", 5, 6), ("r", 2, 3), ("m", 6, 7), ("r", 3, 4),
            ("x", 0, 4),
        ),
        6: (("m", 7, 8), ("r", 4, 5), ("y", 0, 4)),
        7: (("r", 5, 6),),
    }
    late_events = {
        0: (("r", 6, 7), ("x", 4, 6)),
        1: (("y", 4, 6),),
        2: (("r", 7, 8), ("x", 6, 8)),
        3: (("y", 6, 8),),
    }
    actions = {
        "p": lambda c: partner_copy(c).wait_recv(),
        "m": got_mirror, "r": got_rail,
        "x": lambda c: got_cross(c, jnp.logical_not(same)),
        "y": lambda c: got_cross(c, same),
    }

    def run_events(u, table):
        for k, listed in table.items():
            if listed:
                @pl.when(u == k)
                def _():
                    for kind, low_c, high_c in listed:
                        for c in range(low_c, high_c):
                            actions[kind](c)

    def step(u, carry):
        run_events(u, events)
        slot = jnp.where(
            u < 4, u // 2,
            jnp.where(u == 5, late_one, jnp.where(u == 6, late_two, MIRROR)),
        )
        start = jnp.where(u < 4, u % 2, jnp.where(u == 7, 1, 0)) * half
        unit(slot, start, half)

        @pl.when(u < 2 * REACH)
        def _():
            set_bias(u + 1)
        return carry

    lax.fori_loop(0, 8, step, 0)

    def late_step(v, carry):
        run_events(v, late_events)
        slot = jnp.where(v % 2 == 0, late_one, late_two)
        unit(slot, half + (v // 2) * quarter, quarter)
        return carry

    lax.fori_loop(0, 4, late_step, 0)

    for h in range(heads):
        total = acc_ref[h, HEAD_DIM:HEAD_DIM + 1]
        mixed_ref[h * HEAD_DIM:(h + 1) * HEAD_DIM, :] = (
            acc_ref[h, :HEAD_DIM] / total
        ).astype(jnp.bfloat16)
    for load in loads[5:]:
        load.wait()
    after_ref[...] = slab_ref[OWN].astype(jnp.float32) + jnp.dot(
        mixed_ref[...].T, wo_ref[...], preferred_element_type=jnp.float32
    )

    local_mean = jnp.sum(after_ref[...], axis=0, keepdims=True) * (1.0 / rows)
    spread = after_ref[...] - local_mean
    stats_ref[0, 0:1] = local_mean
    stats_ref[0, 1:2] = jnp.sum(spread * spread, axis=0, keepdims=True)

    def stats_copy(d):
        return pltpu.make_async_remote_copy(
            src_ref=stats_ref.at[0], dst_ref=stats_ref.at[d],
            send_sem=s_send.at[d], recv_sem=s_recv.at[d],
            device_id={"blk": lax.rem(me + d, n)}, device_id_type=MESH,
        )

    def send_stats(d, carry):
        stats_copy(d).start()
        return carry

    def take_stats(d, carry):
        stats_copy(d).wait_recv()
        return carry

    lax.fori_loop(1, n, send_stats, 0)

    for c in range(CHUNKS):
        partner_copy(c).wait_send()
        mirror_copy(c).wait_send()
        rail_copy(c).wait_send()
        cross_copy(c, RAIL).wait_send()

    lax.fori_loop(1, n, take_stats, 0)
    gathered = stats_ref[...]
    means = gathered[:, 0, :]
    mean = jnp.sum(means, axis=0, keepdims=True) * (1.0 / n)
    shifts = means - mean
    var = (
        jnp.sum(gathered[:, 1, :], axis=0, keepdims=True) * (1.0 / rows)
        + jnp.sum(shifts * shifts, axis=0, keepdims=True)
    ) * (1.0 / n)
    gain = lax.rsqrt(var + 1e-05) * bg_ref[...]
    batched = ((after_ref[...] - mean) * gain + bs_ref[...]).astype(jnp.bfloat16)
    hidden = jax.nn.gelu(
        jnp.dot(batched, wu_ref[...], preferred_element_type=jnp.float32), approximate=True
    ).astype(jnp.bfloat16)
    out_ref[...] = (
        after_ref[...] + jnp.dot(hidden, wd_ref[...], preferred_element_type=jnp.float32)
    ).astype(jnp.bfloat16)

    def sent_stats(d, carry):
        stats_copy(d).wait_send()
        return carry

    lax.fori_loop(1, n, sent_stats, 0)


def body(
    atoms, edge_mask, norm_gain, w_query, w_key, w_value, w_out, bn_gain, bn_shift, w_up, w_down
):
    n = lax.axis_size("blk")
    rows, width = atoms.shape
    ff = w_up.shape[1]
    slabs = edge_mask.shape[1]
    heads = width // HEAD_DIM
    half = rows // 2
    bf16, f32 = jnp.bfloat16, jnp.float32
    dma = pltpu.SemaphoreType.DMA
    return pl.pallas_call(
        functools.partial(kernel, n),
        out_shape=jax.ShapeDtypeStruct((rows, width), bf16),
        in_specs=[pl.BlockSpec(memory_space=pl.ANY)] * 11,
        out_specs=pl.BlockSpec(memory_space=pltpu.VMEM),
        scratch_shapes=[
            pltpu.VMEM((slabs, rows, width), bf16),
            pltpu.VMEM((slabs, rows, rows), jnp.int32),
            pltpu.VMEM((1, width), f32),
            pltpu.VMEM((width, width), bf16),
            pltpu.VMEM((width, width), bf16),
            pltpu.VMEM((width, width), bf16),
            pltpu.VMEM((width, width), bf16),
            pltpu.VMEM((1, width), f32),
            pltpu.VMEM((1, width), f32),
            pltpu.VMEM((width, ff), bf16),
            pltpu.VMEM((ff, width), bf16),
            pltpu.VMEM((width, width), bf16),
            pltpu.VMEM((heads, 2 * PAIR, rows), bf16),
            pltpu.VMEM((half, width), bf16),
            pltpu.VMEM((heads, HEAD_DIM + SUMS, half), bf16),
            pltpu.VMEM((slabs, rows, rows), f32),
            pltpu.VMEM((heads, 1, rows), f32),
            pltpu.VMEM((heads, HEAD_DIM + SUMS, rows), f32),
            pltpu.VMEM((width, rows), bf16),
            pltpu.VMEM((rows, width), f32),
            pltpu.VMEM((n, 2, width), f32),
            dma((10,)),
            dma((slabs,)),
            dma((CHUNKS,)), dma((CHUNKS,)), dma((CHUNKS,)), dma((CHUNKS,)),
            dma((slabs, CHUNKS)),
            dma((n,)), dma((n,)),
        ],
        compiler_params=pltpu.CompilerParams(
            collective_id=0, has_side_effects=True, vmem_limit_bytes=60 * 1024 * 1024
        ),
    )(
        atoms, edge_mask, norm_gain.reshape(1, width), w_query, w_key, w_value, w_out,
        bn_gain.reshape(1, width), bn_shift.reshape(1, width), w_up, w_down,
    )


def solution(mesh):
    placed = (
        P(("grp", "blk"), None),
        P(("grp", "blk"), None, None, None),
        P(), P(), P(), P(), P(), P(), P(), P(), P(),
    )
    return jax.shard_map(
        body, mesh=mesh, in_specs=placed, out_specs=P(("grp", "blk"), None), check_vma=False
    )
```

```python
import functools
import math

import jax
import jax.numpy as jnp
from jax import lax
from jax.experimental import pallas as pl
from jax.experimental.pallas import tpu as pltpu
from jax.sharding import PartitionSpec as P

HEAD_DIM = 64
PAIR = 2 * HEAD_DIM
REACH = 2
CHUNKS = 8
PARTS = 4
SUMS = 16
LOOK = 3
SLOTS = LOOK + 1
NEG = -1e30
MESH = pl.DeviceIdType.MESH
OWN, PARTNER, MIRROR, RAIL, CROSS = 0, 1, 2, 3, 4
SCALE = math.log2(math.e) * HEAD_DIM ** (-0.5)


def kernel(
    n,
    atoms_hbm, mask_hbm, ng_hbm, wq_hbm, wk_hbm, wv_hbm, wo_hbm, bg_hbm, bs_hbm, wu_hbm, wd_hbm,
    out_ref,
    slab_ref, mask_ref, ng_ref, wq_ref, wk_ref, wv_ref, wo_ref, bg_ref, bs_ref, wu_ref, wd_ref,
    wvt_ref, qt_ref, kb_ref, vt_ref, bias_ref, m_ref, s_ref, acc_ref, mixed_ref, after_ref,
    stats_ref, load_sem, mask_sem,
    p_send, m_send, r_send, c_send, recv, s_send, s_recv, up_sem, down_sem,
):
    me = lax.axis_index("blk")
    rows, width = after_ref.shape
    heads = width // HEAD_DIM
    group, inside = me // 4, me % 4
    side, core = inside // 2, inside % 2
    cousin = group * 4 + (1 - side) * 2 + (1 - core)
    partner = group * 4 + side * 2 + (1 - core)
    mirror = group * 4 + (1 - side) * 2 + core
    groups = n // 4
    rail_to = ((group + 1 - 2 * side + groups) % groups) * 4 + side * 2 + core
    same = side == core
    late_one = jnp.where(same, RAIL, CROSS)
    late_two = jnp.where(same, CROSS, RAIL)

    barrier = pltpu.get_barrier_semaphore()

    for known in (partner, mirror, cousin):
        pl.semaphore_signal(barrier, inc=1, device_id={"blk": known}, device_id_type=MESH)

    @pl.when(group > 0)
    def _():
        pl.semaphore_signal(barrier, inc=1, device_id={"blk": me - 4}, device_id_type=MESH)

    @pl.when(group < groups - 1)
    def _():
        pl.semaphore_signal(barrier, inc=1, device_id={"blk": me + 4}, device_id_type=MESH)

    def tell_up():
        @pl.when(group < groups - 1)
        def _():
            pl.semaphore_signal(up_sem, inc=1, device_id={"blk": me + 4}, device_id_type=MESH)

    def tell_down():
        @pl.when(group > 0)
        def _():
            pl.semaphore_signal(down_sem, inc=1, device_id={"blk": me - 4}, device_id_type=MESH)

    def roll_call_start():
        @pl.when(group == 0)
        def _():
            tell_up()

        @pl.when(group == groups - 1)
        def _():
            tell_down()

    def roll_call_early():
        @pl.when(group == 1)
        def _():
            pl.semaphore_wait(up_sem, 1)
            tell_up()

        @pl.when(group == groups - 2)
        def _():
            pl.semaphore_wait(down_sem, 1)
            tell_down()

    def roll_call_end():
        @pl.when(group > 1)
        def _():
            pl.semaphore_wait(up_sem, 1)
            tell_up()

        @pl.when(group < groups - 2)
        def _():
            pl.semaphore_wait(down_sem, 1)
            tell_down()

    sources = (
        (atoms_hbm, slab_ref.at[OWN]), (ng_hbm, ng_ref.at[0:1]), (wq_hbm, wq_ref), (wk_hbm, wk_ref),
        (wv_hbm, wv_ref), (wo_hbm, wo_ref), (bg_hbm, bg_ref.at[0:1]), (bs_hbm, bs_ref.at[0:1]),
        (wu_hbm, wu_ref), (wd_hbm, wd_ref),
    )
    loads = [
        pltpu.make_async_copy(src, dst, load_sem.at[i]) for i, (src, dst) in enumerate(sources)
    ]
    far = jnp.where(side == 0, 2, -2)
    near = jnp.where(core == 0, 1, -1)
    offsets = [jnp.int32(0), near, far, -far, -near]
    masks = [
        pltpu.make_async_copy(
            mask_hbm.at[0, offsets[i] + REACH], mask_ref.at[i], mask_sem.at[i]
        )
        for i in range(2 * REACH + 1)
    ]
    for i in range(5):
        loads[i].start()
    for mask_load in masks:
        mask_load.start()
    for i in range(5, len(loads)):
        loads[i].start()

    step_rows = rows // CHUNKS

    def chunk(c):
        return pl.ds(c * step_rows, step_rows)

    def copy(source, target, c, sem, device):
        return pltpu.make_async_remote_copy(
            src_ref=slab_ref.at[source, chunk(c)], dst_ref=slab_ref.at[target, chunk(c)],
            send_sem=sem.at[c], recv_sem=recv.at[target, c],
            device_id={"blk": device}, device_id_type=MESH,
        )

    def partner_copy(c):
        return copy(OWN, PARTNER, c, p_send, partner)

    def mirror_copy(c):
        return copy(OWN, MIRROR, c, m_send, mirror)

    def rail_copy(c):
        return copy(MIRROR, RAIL, c, r_send, rail_to)

    def cross_copy(c, source):
        return copy(source, CROSS, c, c_send, partner)

    def got_mirror(c):
        mirror_copy(c).wait_recv()
        rail_copy(c).start()

        @pl.when(same)
        def _():
            cross_copy(c, MIRROR).start()

    def got_rail(c):
        rail_copy(c).wait_recv()

        @pl.when(jnp.logical_not(same))
        def _():
            cross_copy(c, RAIL).start()

    def got_cross(c, when):
        @pl.when(when)
        def _():
            cross_copy(c, RAIL).wait_recv()

    loads[0].wait()
    pl.semaphore_wait(
        barrier, 3 + (group > 0).astype(jnp.int32) + (group < groups - 1).astype(jnp.int32)
    )
    for c in range(CHUNKS):
        mirror_copy(c).start()
    for c in range(CHUNKS):
        partner_copy(c).start()
    roll_call_start()

    def normalize(value):
        full = value.astype(jnp.float32)
        return (
            full * lax.rsqrt(jnp.mean(full * full, axis=-1, keepdims=True) + 1e-06) * ng_ref[0:1]
        ).astype(jnp.bfloat16)

    def set_bias(i):
        @pl.when(i == 0)
        def _():
            masks[0].wait()

        for j in range(1, 2 * REACH + 1):
            @pl.when(i == j)
            def _():
                masks[j].wait()

        for k in range(rows // PAIR):
            span = slice(k * PAIR, (k + 1) * PAIR)
            bias_ref[i, span, :] = jnp.where(mask_ref[i, :, span] > 0, 0.0, NEG).T

    def unit(slot, start, count):
        normed = normalize(slab_ref[slot, pl.ds(start, count), :])
        kb_ref[:count] = jnp.dot(
            normed, wk_ref[...], preferred_element_type=jnp.float32
        ).astype(jnp.bfloat16)
        values = lax.dot_general(
            wvt_ref[...], normed, (((1,), (1,)), ((), ())), preferred_element_type=jnp.float32
        ).astype(jnp.bfloat16)
        for h in range(heads):
            vt_ref[h, :HEAD_DIM, :count] = values[h * HEAD_DIM:(h + 1) * HEAD_DIM]

        def scores(h):
            pair = h // 2
            piece = kb_ref[:count, pair * PAIR:(pair + 1) * PAIR]
            score = jnp.dot(
                jnp.concatenate([piece, piece], axis=1), qt_ref[h],
                preferred_element_type=jnp.float32,
            ) + bias_ref[slot, pl.ds(start, count), :]
            s_ref[h % SLOTS, :count] = score
            return jnp.max(score, axis=0, keepdims=True)

        def finish(h, peak):
            old = m_ref[h, 0:1]
            new = jnp.maximum(old, peak)
            m_ref[h, 0:1] = new
            weight = jnp.exp2(s_ref[h % SLOTS, :count] - new).astype(jnp.bfloat16)
            result = jnp.dot(vt_ref[h, :, :count], weight, preferred_element_type=jnp.float32)
            acc_ref[h] = acc_ref[h] * jnp.exp2(old - new) + result

        peaks = [scores(h) for h in range(LOOK)]
        for h in range(heads):
            if h + LOOK < heads:
                peaks.append(scores(h + LOOK))
            finish(h, peaks[h])

    ones = jnp.ones((heads, SUMS, vt_ref.shape[2]), jnp.bfloat16)
    vt_ref[:, HEAD_DIM:, :] = ones
    m_ref[...] = jnp.full(m_ref.shape, NEG, jnp.float32)
    acc_ref[...] = jnp.zeros(acc_ref.shape, jnp.float32)

    loads[1].wait()
    normed = normalize(slab_ref[OWN])
    loads[2].wait()
    wqt = wq_ref[...].T
    query = lax.dot_general(
        wqt, normed, (((1,), (1,)), ((), ())), preferred_element_type=jnp.float32
    ).astype(jnp.bfloat16).astype(jnp.float32) * SCALE
    high = query.astype(jnp.bfloat16)
    low = (query - high.astype(jnp.float32)).astype(jnp.bfloat16)
    zero = jnp.zeros((HEAD_DIM, rows), jnp.bfloat16)
    for h in range(heads):
        span = slice(h * HEAD_DIM, (h + 1) * HEAD_DIM)
        for part, base in ((high, 0), (low, PAIR)):
            here = base + (h % 2) * HEAD_DIM
            there = base + (1 - h % 2) * HEAD_DIM
            qt_ref[h, here:here + HEAD_DIM] = part[span]
            qt_ref[h, there:there + HEAD_DIM] = zero
    roll_call_early()
    loads[4].wait()
    wvt_ref[...] = wv_ref[...].T
    loads[3].wait()
    set_bias(0)
    eye = lax.broadcasted_iota(jnp.int32, (rows, rows), 0) == lax.broadcasted_iota(
        jnp.int32, (rows, rows), 1
    )
    bias_ref[0] = jnp.where(eye, 0.0, bias_ref[0])

    def more_bias(i, carry):
        set_bias(i)
        return carry

    lax.fori_loop(1, 2 * REACH + 1, more_bias, 0)

    roll_call_end()
    half = rows // 2
    quarter = rows // PARTS

    events = {
        0: (),
        1: (),
        2: (("p", 0, 8),),
        3: (("m", 0, 1),),
        4: (("m", 1, 4), ("r", 0, 1)),
        5: (
            ("m", 4, 5), ("r", 1, 2), ("m", 5, 6), ("r", 2, 3), ("m", 6, 7), ("r", 3, 4),
            ("x", 0, 4),
        ),
        6: (("m", 7, 8), ("r", 4, 5), ("y", 0, 4)),
        7: (("r", 5, 6),),
    }
    late_events = {
        0: (("r", 6, 7), ("x", 4, 6)),
        1: (("y", 4, 6),),
        2: (("r", 7, 8), ("x", 6, 8)),
        3: (("y", 6, 8),),
    }
    actions = {
        "p": lambda c: partner_copy(c).wait_recv(),
        "m": got_mirror, "r": got_rail,
        "x": lambda c: got_cross(c, jnp.logical_not(same)),
        "y": lambda c: got_cross(c, same),
    }

    def run_events(u, table):
        for k, listed in table.items():
            if listed:
                @pl.when(u == k)
                def _():
                    for kind, low_c, high_c in listed:
                        for c in range(low_c, high_c):
                            actions[kind](c)

    def step(u, carry):
        run_events(u, events)
        slot = jnp.where(
            u < 4, u // 2,
            jnp.where(u == 5, late_one, jnp.where(u == 6, late_two, MIRROR)),
        )
        start = jnp.where(u < 4, u % 2, jnp.where(u == 7, 1, 0)) * half
        unit(slot, start, half)
        return carry

    lax.fori_loop(0, 8, step, 0)

    def late_step(v, carry):
        run_events(v, late_events)
        slot = jnp.where(v % 2 == 0, late_one, late_two)
        unit(slot, half + (v // 2) * quarter, quarter)
        return carry

    lax.fori_loop(0, 4, late_step, 0)

    for h in range(heads):
        total = acc_ref[h, HEAD_DIM:HEAD_DIM + 1]
        mixed_ref[h * HEAD_DIM:(h + 1) * HEAD_DIM, :] = (
            acc_ref[h, :HEAD_DIM] / total
        ).astype(jnp.bfloat16)
    for load in loads[5:]:
        load.wait()
    after_ref[...] = slab_ref[OWN].astype(jnp.float32) + jnp.dot(
        mixed_ref[...].T, wo_ref[...], preferred_element_type=jnp.float32
    )

    local_mean = jnp.sum(after_ref[...], axis=0, keepdims=True) * (1.0 / rows)
    spread = after_ref[...] - local_mean
    stats_ref[0, 0:1] = local_mean
    stats_ref[0, 1:2] = jnp.sum(spread * spread, axis=0, keepdims=True)

    def stats_copy(d):
        return pltpu.make_async_remote_copy(
            src_ref=stats_ref.at[0], dst_ref=stats_ref.at[d],
            send_sem=s_send.at[d], recv_sem=s_recv.at[d],
            device_id={"blk": lax.rem(me + d, n)}, device_id_type=MESH,
        )

    def send_stats(d, carry):
        stats_copy(d).start()
        return carry

    def take_stats(d, carry):
        stats_copy(d).wait_recv()
        return carry

    lax.fori_loop(1, n, send_stats, 0)

    for c in range(CHUNKS):
        partner_copy(c).wait_send()
        mirror_copy(c).wait_send()
        rail_copy(c).wait_send()
        cross_copy(c, RAIL).wait_send()

    lax.fori_loop(1, n, take_stats, 0)
    gathered = stats_ref[...]
    means = gathered[:, 0, :]
    mean = jnp.sum(means, axis=0, keepdims=True) * (1.0 / n)
    shifts = means - mean
    var = (
        jnp.sum(gathered[:, 1, :], axis=0, keepdims=True) * (1.0 / rows)
        + jnp.sum(shifts * shifts, axis=0, keepdims=True)
    ) * (1.0 / n)
    gain = lax.rsqrt(var + 1e-05) * bg_ref[0:1]
    batched = ((after_ref[...] - mean) * gain + bs_ref[0:1]).astype(jnp.bfloat16)
    hidden = jax.nn.gelu(
        jnp.dot(batched, wu_ref[...], preferred_element_type=jnp.float32), approximate=True
    ).astype(jnp.bfloat16)
    out_ref[...] = (
        after_ref[...] + jnp.dot(hidden, wd_ref[...], preferred_element_type=jnp.float32)
    ).astype(jnp.bfloat16)

    def sent_stats(d, carry):
        stats_copy(d).wait_send()
        return carry

    lax.fori_loop(1, n, sent_stats, 0)


def body(
    atoms, edge_mask, norm_gain, w_query, w_key, w_value, w_out, bn_gain, bn_shift, w_up, w_down
):
    n = lax.axis_size("blk")
    rows, width = atoms.shape
    ff = w_up.shape[1]
    slabs = edge_mask.shape[1]
    heads = width // HEAD_DIM
    half = rows // 2
    bf16, f32 = jnp.bfloat16, jnp.float32
    dma = pltpu.SemaphoreType.DMA
    return pl.pallas_call(
        functools.partial(kernel, n),
        out_shape=pltpu.VMEM((rows, width), bf16),
        in_specs=[pl.BlockSpec(memory_space=pl.ANY)] * 11,
        out_specs=pl.BlockSpec(memory_space=pltpu.VMEM),
        scratch_shapes=[
            pltpu.VMEM((slabs, rows, width), bf16),
            pltpu.VMEM((slabs, rows, rows), jnp.int32),
            pltpu.VMEM((8, width), f32),
            pltpu.VMEM((width, width), bf16),
            pltpu.VMEM((width, width), bf16),
            pltpu.VMEM((width, width), bf16),
            pltpu.VMEM((width, width), bf16),
            pltpu.VMEM((8, width), f32),
            pltpu.VMEM((8, width), f32),
            pltpu.VMEM((width, ff), bf16),
            pltpu.VMEM((ff, width), bf16),
            pltpu.VMEM((width, width), bf16),
            pltpu.VMEM((heads, 2 * PAIR, rows), bf16),
            pltpu.VMEM((half, width), bf16),
            pltpu.VMEM((heads, HEAD_DIM + SUMS, half), bf16),
            pltpu.VMEM((slabs, rows, rows), f32),
            pltpu.VMEM((heads, 8, rows), f32),
            pltpu.VMEM((SLOTS, half, rows), f32),
            pltpu.VMEM((heads, HEAD_DIM + SUMS, rows), f32),
            pltpu.VMEM((width, rows), bf16),
            pltpu.VMEM((rows, width), f32),
            pltpu.VMEM((n, 2, width), f32),
            dma((10,)),
            dma((slabs,)),
            dma((CHUNKS,)), dma((CHUNKS,)), dma((CHUNKS,)), dma((CHUNKS,)),
            dma((slabs, CHUNKS)),
            dma((n,)), dma((n,)),
            pltpu.SemaphoreType.REGULAR, pltpu.SemaphoreType.REGULAR,
        ],
        compiler_params=pltpu.CompilerParams(
            collective_id=0, has_side_effects=True, vmem_limit_bytes=60 * 1024 * 1024
        ),
    )(
        atoms, edge_mask, norm_gain.reshape(1, width), w_query, w_key, w_value, w_out,
        bn_gain.reshape(1, width), bn_shift.reshape(1, width), w_up, w_down,
    )


def solution(mesh):
    placed = (
        P(("grp", "blk"), None),
        P(("grp", "blk"), None, None, None),
        P(), P(), P(), P(), P(), P(), P(), P(), P(),
    )
    return jax.shard_map(
        body, mesh=mesh, in_specs=placed, out_specs=P(("grp", "blk"), None), check_vma=False
    )
```

```python
import functools
import math

import jax
import jax.numpy as jnp
from jax import lax
from jax.experimental import pallas as pl
from jax.experimental.pallas import tpu as pltpu
from jax.sharding import PartitionSpec as P

HEAD_DIM = 64
PAIR = 2 * HEAD_DIM
REACH = 2
CHUNKS = 8
SUMS = 16
LOOK = 3
SLOTS = LOOK + 1
NEG = -1e30
MESH = pl.DeviceIdType.MESH
OWN, PARTNER, MIRROR, RAIL, CROSS = 0, 1, 2, 3, 4
SCALE = math.log2(math.e) * HEAD_DIM ** (-0.5)


def kernel(
    n,
    atoms_hbm, mask_hbm, ng_hbm, wq_hbm, wk_hbm, wv_hbm, wo_hbm, bg_hbm, bs_hbm, wu_hbm, wd_hbm,
    out_ref,
    slab_ref, mask_ref, ng_ref, wq_ref, wk_ref, wv_ref, wo_ref, bg_ref, bs_ref, wu_ref, wd_ref,
    wvt_ref, qt_ref, normed_ref, kb_ref, vt_ref, bias_ref, m_ref, s_ref, acc_ref, mixed_ref, after_ref,
    stats_ref, load_sem, mask_sem,
    p_send, m_send, r_send, c_send, recv, s_send, s_recv, up_sem, down_sem,
):
    me = lax.axis_index("blk")
    rows, width = after_ref.shape
    heads = width // HEAD_DIM
    group, inside = me // 4, me % 4
    side, core = inside // 2, inside % 2
    cousin = group * 4 + (1 - side) * 2 + (1 - core)
    partner = group * 4 + side * 2 + (1 - core)
    mirror = group * 4 + (1 - side) * 2 + core
    groups = n // 4
    rail_to = ((group + 1 - 2 * side + groups) % groups) * 4 + side * 2 + core
    same = side == core
    late_one = jnp.where(same, RAIL, CROSS)
    late_two = jnp.where(same, CROSS, RAIL)

    barrier = pltpu.get_barrier_semaphore()

    for known in (partner, mirror, cousin):
        pl.semaphore_signal(barrier, inc=1, device_id={"blk": known}, device_id_type=MESH)

    @pl.when(group > 0)
    def _():
        pl.semaphore_signal(barrier, inc=1, device_id={"blk": me - 4}, device_id_type=MESH)

    @pl.when(group < groups - 1)
    def _():
        pl.semaphore_signal(barrier, inc=1, device_id={"blk": me + 4}, device_id_type=MESH)

    def tell_up():
        @pl.when(group < groups - 1)
        def _():
            pl.semaphore_signal(up_sem, inc=1, device_id={"blk": me + 4}, device_id_type=MESH)

    def tell_down():
        @pl.when(group > 0)
        def _():
            pl.semaphore_signal(down_sem, inc=1, device_id={"blk": me - 4}, device_id_type=MESH)

    def roll_call_start():
        @pl.when(group == 0)
        def _():
            tell_up()

        @pl.when(group == groups - 1)
        def _():
            tell_down()

    def roll_call_early():
        @pl.when(group == 1)
        def _():
            pl.semaphore_wait(up_sem, 1)
            tell_up()

        @pl.when(group == groups - 2)
        def _():
            pl.semaphore_wait(down_sem, 1)
            tell_down()

    def roll_call_end():
        @pl.when(group > 1)
        def _():
            pl.semaphore_wait(up_sem, 1)
            tell_up()

        @pl.when(group < groups - 2)
        def _():
            pl.semaphore_wait(down_sem, 1)
            tell_down()

    sources = (
        (atoms_hbm, slab_ref.at[OWN]), (ng_hbm, ng_ref.at[0:1]), (wq_hbm, wq_ref), (wk_hbm, wk_ref),
        (wv_hbm, wv_ref), (wo_hbm, wo_ref), (bg_hbm, bg_ref.at[0:1]), (bs_hbm, bs_ref.at[0:1]),
        (wu_hbm, wu_ref), (wd_hbm, wd_ref),
    )
    loads = [
        pltpu.make_async_copy(src, dst, load_sem.at[i]) for i, (src, dst) in enumerate(sources)
    ]
    far = jnp.where(side == 0, 2, -2)
    near = jnp.where(core == 0, 1, -1)
    offsets = [jnp.int32(0), near, far, -far, -near]
    masks = [
        pltpu.make_async_copy(
            mask_hbm.at[0, offsets[i] + REACH], mask_ref.at[i], mask_sem.at[i]
        )
        for i in range(2 * REACH + 1)
    ]
    for i in range(5):
        loads[i].start()
    for mask_load in masks:
        mask_load.start()
    for i in range(5, len(loads)):
        loads[i].start()

    step_rows = rows // CHUNKS

    def chunk(c):
        return pl.ds(c * step_rows, step_rows)

    def copy(source, target, c, sem, device):
        return pltpu.make_async_remote_copy(
            src_ref=slab_ref.at[source, chunk(c)], dst_ref=slab_ref.at[target, chunk(c)],
            send_sem=sem.at[c], recv_sem=recv.at[target, c],
            device_id={"blk": device}, device_id_type=MESH,
        )

    def partner_copy(c):
        return copy(OWN, PARTNER, c, p_send, partner)

    def mirror_copy(c):
        return copy(OWN, MIRROR, c, m_send, mirror)

    def rail_copy(c):
        return copy(MIRROR, RAIL, c, r_send, rail_to)

    def cross_copy(c, source):
        return copy(source, CROSS, c, c_send, partner)

    def got_mirror(c):
        mirror_copy(c).wait_recv()
        rail_copy(c).start()

        @pl.when(same)
        def _():
            cross_copy(c, MIRROR).start()

    def got_rail(c):
        rail_copy(c).wait_recv()

        @pl.when(jnp.logical_not(same))
        def _():
            cross_copy(c, RAIL).start()

    def got_cross(c, when):
        @pl.when(when)
        def _():
            cross_copy(c, RAIL).wait_recv()

    loads[0].wait()
    pl.semaphore_wait(
        barrier, 3 + (group > 0).astype(jnp.int32) + (group < groups - 1).astype(jnp.int32)
    )
    for c in range(CHUNKS):
        mirror_copy(c).start()
    for c in range(CHUNKS):
        partner_copy(c).start()
    roll_call_start()

    def normalize(value):
        full = value.astype(jnp.float32)
        return (
            full * lax.rsqrt(jnp.mean(full * full, axis=-1, keepdims=True) + 1e-06) * ng_ref[0:1]
        ).astype(jnp.bfloat16)

    def unit(pieces, count):
        total = len(pieces) * count
        for i, (slot, start) in enumerate(pieces):
            normed_ref[i * count:(i + 1) * count] = normalize(
                slab_ref[slot, pl.ds(start, count), :]
            )
        kb_ref[...] = jnp.dot(
            normed_ref[...], wk_ref[...], preferred_element_type=jnp.float32
        ).astype(jnp.bfloat16)
        values = lax.dot_general(
            wvt_ref[...], normed_ref[...], (((1,), (1,)), ((), ())),
            preferred_element_type=jnp.float32,
        ).astype(jnp.bfloat16)
        for h in range(heads):
            vt_ref[h, :HEAD_DIM] = values[h * HEAD_DIM:(h + 1) * HEAD_DIM]
        atom = lax.broadcasted_iota(jnp.int32, (rows, PAIR), 0)
        other = lax.broadcasted_iota(jnp.int32, (rows, PAIR), 1)
        for i, (slot, start) in enumerate(pieces):
            linked = mask_ref[slot, :, pl.ds(pl.multiple_of(start, PAIR), PAIR)] > 0
            shift = start + jnp.where(slot == OWN, 0, rows)
            bias_ref[i * count:(i + 1) * count, :] = jnp.where(
                linked | (atom == other + shift), 0.0, NEG
            ).T

        def scores(h):
            pair = h // 2
            piece = kb_ref[:total, pair * PAIR:(pair + 1) * PAIR]
            score = jnp.dot(
                jnp.concatenate([piece, piece], axis=1), qt_ref[h],
                preferred_element_type=jnp.float32,
            ) + bias_ref[:total]
            s_ref[h % SLOTS, :total] = score
            return jnp.max(score, axis=0, keepdims=True)

        def finish(h, peak):
            old = m_ref[h, 0:1]
            new = jnp.maximum(old, peak)
            m_ref[h, 0:1] = new
            weight = jnp.exp2(s_ref[h % SLOTS, :total] - new).astype(jnp.bfloat16)
            result = jnp.dot(vt_ref[h, :, :total], weight, preferred_element_type=jnp.float32)
            acc_ref[h] = acc_ref[h] * jnp.exp2(old - new) + result

        peaks = [scores(h) for h in range(LOOK)]
        for h in range(heads):
            if h + LOOK < heads:
                peaks.append(scores(h + LOOK))
            finish(h, peaks[h])

    ones = jnp.ones((heads, SUMS, vt_ref.shape[2]), jnp.bfloat16)
    vt_ref[:, HEAD_DIM:, :] = ones
    m_ref[...] = jnp.full(m_ref.shape, NEG, jnp.float32)
    acc_ref[...] = jnp.zeros(acc_ref.shape, jnp.float32)

    loads[1].wait()
    normed = normalize(slab_ref[OWN])
    loads[2].wait()
    wqt = wq_ref[...].T
    query = lax.dot_general(
        wqt, normed, (((1,), (1,)), ((), ())), preferred_element_type=jnp.float32
    ).astype(jnp.bfloat16).astype(jnp.float32) * SCALE
    high = query.astype(jnp.bfloat16)
    low = (query - high.astype(jnp.float32)).astype(jnp.bfloat16)
    zero = jnp.zeros((HEAD_DIM, rows), jnp.bfloat16)
    for h in range(heads):
        span = slice(h * HEAD_DIM, (h + 1) * HEAD_DIM)
        for part, base in ((high, 0), (low, PAIR)):
            here = base + (h % 2) * HEAD_DIM
            there = base + (1 - h % 2) * HEAD_DIM
            qt_ref[h, here:here + HEAD_DIM] = part[span]
            qt_ref[h, there:there + HEAD_DIM] = zero
    roll_call_early()
    loads[4].wait()
    wvt_ref[...] = wv_ref[...].T
    loads[3].wait()

    actions = {
        "p": lambda c: partner_copy(c).wait_recv(),
        "e": lambda c: roll_call_end(),
        "m": got_mirror, "r": got_rail,
        "x": lambda c: got_cross(c, jnp.logical_not(same)),
        "y": lambda c: got_cross(c, same),
    }

    def run(listed):
        for kind, low_c, high_c in listed:
            for c in range(low_c, high_c):
                actions[kind](c)

    def run_events(u, table):
        for k, listed in table.items():
            @pl.when(u == k)
            def _():
                run(listed)

    half = rows // 2

    def step(u, carry):
        run_events(u, {
            1: (("e", 0, 1), ("m", 0, 1)),
            2: (("p", 0, 8), ("m", 1, 2)),
            3: (("m", 2, 3),),
            4: (("m", 3, 4),),
            5: (
                ("m", 4, 5), ("r", 0, 1), ("m", 5, 6), ("r", 1, 3), ("m", 6, 7), ("r", 3, 4),
                ("x", 0, 4),
            ),
            6: (("m", 7, 8), ("r", 4, 5), ("y", 0, 4)),
            7: (("r", 5, 6),),
            8: (("r", 6, 7), ("x", 4, 6), ("y", 4, 6)),
            9: (("r", 7, 8), ("x", 6, 8), ("y", 6, 8)),
        })
        for k, listed in ((0, (0,)), (2, (1,)), (4, (2,)), (5, (3, 4))):
            @pl.when(u == k)
            def _():
                for i in listed:
                    masks[i].wait()
        slot = jnp.where(
            u < 4, u // 2,
            jnp.where((u == 4) | (u == 7), MIRROR, jnp.where(u == 6, late_two, late_one)),
        )
        start = jnp.where(
            u < 4, (u % 2) * half,
            jnp.where(u < 7, 0, half + jnp.where(u == 9, PAIR, 0)),
        )
        slot_too = jnp.where(u < 8, slot, late_two)
        start_too = jnp.where(u < 8, start + PAIR, start)
        unit([(slot, start), (slot_too, start_too)], PAIR)
        return carry

    lax.fori_loop(0, 5, step, 0)
    lax.fori_loop(5, 10, step, 0)

    for h in range(heads):
        total = acc_ref[h, HEAD_DIM:HEAD_DIM + 1]
        mixed_ref[h * HEAD_DIM:(h + 1) * HEAD_DIM, :] = (
            acc_ref[h, :HEAD_DIM] / total
        ).astype(jnp.bfloat16)
    for load in loads[5:]:
        load.wait()
    after_ref[...] = slab_ref[OWN].astype(jnp.float32) + jnp.dot(
        mixed_ref[...].T, wo_ref[...], preferred_element_type=jnp.float32
    )

    local_mean = jnp.sum(after_ref[...], axis=0, keepdims=True) * (1.0 / rows)
    spread = after_ref[...] - local_mean
    stats_ref[0, 0:1] = local_mean
    stats_ref[0, 1:2] = jnp.sum(spread * spread, axis=0, keepdims=True)

    def stats_copy(d):
        return pltpu.make_async_remote_copy(
            src_ref=stats_ref.at[0], dst_ref=stats_ref.at[d],
            send_sem=s_send.at[d], recv_sem=s_recv.at[d],
            device_id={"blk": lax.rem(me + d, n)}, device_id_type=MESH,
        )

    def send_stats(d, carry):
        stats_copy(d).start()
        return carry

    def take_stats(d, carry):
        stats_copy(d).wait_recv()
        return carry

    lax.fori_loop(1, n, send_stats, 0)

    for c in range(CHUNKS):
        partner_copy(c).wait_send()
        mirror_copy(c).wait_send()
        rail_copy(c).wait_send()
        cross_copy(c, RAIL).wait_send()

    lax.fori_loop(1, n, take_stats, 0)
    gathered = stats_ref[...]
    means = gathered[:, 0, :]
    mean = jnp.sum(means, axis=0, keepdims=True) * (1.0 / n)
    shifts = means - mean
    var = (
        jnp.sum(gathered[:, 1, :], axis=0, keepdims=True) * (1.0 / rows)
        + jnp.sum(shifts * shifts, axis=0, keepdims=True)
    ) * (1.0 / n)
    gain = lax.rsqrt(var + 1e-05) * bg_ref[0:1]
    batched = ((after_ref[...] - mean) * gain + bs_ref[0:1]).astype(jnp.bfloat16)
    hidden = jax.nn.gelu(
        jnp.dot(batched, wu_ref[...], preferred_element_type=jnp.float32), approximate=True
    ).astype(jnp.bfloat16)
    out_ref[...] = (
        after_ref[...] + jnp.dot(hidden, wd_ref[...], preferred_element_type=jnp.float32)
    ).astype(jnp.bfloat16)

    def sent_stats(d, carry):
        stats_copy(d).wait_send()
        return carry

    lax.fori_loop(1, n, sent_stats, 0)


def body(
    atoms, edge_mask, norm_gain, w_query, w_key, w_value, w_out, bn_gain, bn_shift, w_up, w_down
):
    n = lax.axis_size("blk")
    rows, width = atoms.shape
    ff = w_up.shape[1]
    slabs = edge_mask.shape[1]
    heads = width // HEAD_DIM
    bf16, f32 = jnp.bfloat16, jnp.float32
    dma = pltpu.SemaphoreType.DMA
    return pl.pallas_call(
        functools.partial(kernel, n),
        out_shape=pltpu.VMEM((rows, width), bf16),
        in_specs=[pl.BlockSpec(memory_space=pl.ANY)] * 11,
        out_specs=pl.BlockSpec(memory_space=pltpu.VMEM),
        scratch_shapes=[
            pltpu.VMEM((slabs, rows, width), bf16),
            pltpu.VMEM((slabs, rows, rows), jnp.int32),
            pltpu.VMEM((8, width), f32),
            pltpu.VMEM((width, width), bf16),
            pltpu.VMEM((width, width), bf16),
            pltpu.VMEM((width, width), bf16),
            pltpu.VMEM((width, width), bf16),
            pltpu.VMEM((8, width), f32),
            pltpu.VMEM((8, width), f32),
            pltpu.VMEM((width, ff), bf16),
            pltpu.VMEM((ff, width), bf16),
            pltpu.VMEM((width, width), bf16),
            pltpu.VMEM((heads, 2 * PAIR, rows), bf16),
            pltpu.VMEM((2 * PAIR, width), bf16),
            pltpu.VMEM((2 * PAIR, width), bf16),
            pltpu.VMEM((heads, HEAD_DIM + SUMS, 2 * PAIR), bf16),
            pltpu.VMEM((2 * PAIR, rows), f32),
            pltpu.VMEM((heads, 8, rows), f32),
            pltpu.VMEM((SLOTS, 2 * PAIR, rows), f32),
            pltpu.VMEM((heads, HEAD_DIM + SUMS, rows), f32),
            pltpu.VMEM((width, rows), bf16),
            pltpu.VMEM((rows, width), f32),
            pltpu.VMEM((n, 2, width), f32),
            dma((10,)),
            dma((slabs,)),
            dma((CHUNKS,)), dma((CHUNKS,)), dma((CHUNKS,)), dma((CHUNKS,)),
            dma((slabs, CHUNKS)),
            dma((n,)), dma((n,)),
            pltpu.SemaphoreType.REGULAR, pltpu.SemaphoreType.REGULAR,
        ],
        compiler_params=pltpu.CompilerParams(
            collective_id=0, has_side_effects=True, vmem_limit_bytes=60 * 1024 * 1024
        ),
    )(
        atoms, edge_mask, norm_gain.reshape(1, width), w_query, w_key, w_value, w_out,
        bn_gain.reshape(1, width), bn_shift.reshape(1, width), w_up, w_down,
    )


def solution(mesh):
    placed = (
        P(("grp", "blk"), None),
        P(("grp", "blk"), None, None, None),
        P(), P(), P(), P(), P(), P(), P(), P(), P(),
    )
    return jax.shard_map(
        body, mesh=mesh, in_specs=placed, out_specs=P(("grp", "blk"), None), check_vma=False
    )
```

```python
import functools
import math

import jax
import jax.numpy as jnp
from jax import lax
from jax.experimental import pallas as pl
from jax.experimental.pallas import tpu as pltpu
from jax.sharding import PartitionSpec as P

HEAD_DIM = 64
PAIR = 2 * HEAD_DIM
REACH = 2
CHUNKS = 8
SUMS = 16
LOOK = 3
SLOTS = LOOK + 1
NEG = -1e30
MESH = pl.DeviceIdType.MESH
OWN, PARTNER, MIRROR, RAIL, CROSS = 0, 1, 2, 3, 4
SCALE = math.log2(math.e) * HEAD_DIM ** (-0.5)


def kernel(
    n,
    atoms_hbm, mask_hbm, ng_hbm, wq_hbm, wk_hbm, wv_hbm, wo_hbm, bg_hbm, bs_hbm, wu_hbm, wd_hbm,
    out_ref,
    slab_ref, mask_ref, ng_ref, wq_ref, wk_ref, wv_ref, wo_ref, bg_ref, bs_ref, wu_ref, wd_ref,
    wvt_ref, qt_ref, normed_ref, kb_ref, vt_ref, bias_ref, m_ref, s_ref, acc_ref, mixed_ref, after_ref,
    stats_ref, load_sem, mask_sem,
    p_send, p_recv, m_send, r_send, c_send, recv, s_send, s_recv, up_sem, down_sem,
):
    me = lax.axis_index("blk")
    rows, width = after_ref.shape
    heads = width // HEAD_DIM
    group, inside = me // 4, me % 4
    side, core = inside // 2, inside % 2
    cousin = group * 4 + (1 - side) * 2 + (1 - core)
    partner = group * 4 + side * 2 + (1 - core)
    mirror = group * 4 + (1 - side) * 2 + core
    groups = n // 4
    rail_to = ((group + 1 - 2 * side + groups) % groups) * 4 + side * 2 + core
    same = side == core

    barrier = pltpu.get_barrier_semaphore()

    for known in (partner, mirror, cousin):
        pl.semaphore_signal(barrier, inc=1, device_id={"blk": known}, device_id_type=MESH)

    @pl.when(group > 0)
    def _():
        pl.semaphore_signal(barrier, inc=1, device_id={"blk": me - 4}, device_id_type=MESH)

    @pl.when(group < groups - 1)
    def _():
        pl.semaphore_signal(barrier, inc=1, device_id={"blk": me + 4}, device_id_type=MESH)

    def tell_up():
        @pl.when(group < groups - 1)
        def _():
            pl.semaphore_signal(up_sem, inc=1, device_id={"blk": me + 4}, device_id_type=MESH)

    def tell_down():
        @pl.when(group > 0)
        def _():
            pl.semaphore_signal(down_sem, inc=1, device_id={"blk": me - 4}, device_id_type=MESH)

    def roll_call_start():
        @pl.when(group == 0)
        def _():
            tell_up()

        @pl.when(group == groups - 1)
        def _():
            tell_down()

    def roll_call_early():
        @pl.when(group == 1)
        def _():
            pl.semaphore_wait(up_sem, 1)
            tell_up()

        @pl.when(group == groups - 2)
        def _():
            pl.semaphore_wait(down_sem, 1)
            tell_down()

    def roll_call_end():
        @pl.when(group > 1)
        def _():
            pl.semaphore_wait(up_sem, 1)
            tell_up()

        @pl.when(group < groups - 2)
        def _():
            pl.semaphore_wait(down_sem, 1)
            tell_down()

    sources = (
        (atoms_hbm, slab_ref.at[OWN]), (ng_hbm, ng_ref.at[0:1]), (wq_hbm, wq_ref), (wk_hbm, wk_ref),
        (wv_hbm, wv_ref), (wo_hbm, wo_ref), (bg_hbm, bg_ref.at[0:1]), (bs_hbm, bs_ref.at[0:1]),
        (wu_hbm, wu_ref), (wd_hbm, wd_ref),
    )
    loads = [
        pltpu.make_async_copy(src, dst, load_sem.at[i]) for i, (src, dst) in enumerate(sources)
    ]
    far = jnp.where(side == 0, 2, -2)
    near = jnp.where(core == 0, 1, -1)
    offsets = [jnp.int32(0), near, far, -far, -near]
    masks = [
        pltpu.make_async_copy(
            mask_hbm.at[0, offsets[i] + REACH], mask_ref.at[i], mask_sem.at[i]
        )
        for i in range(2 * REACH + 1)
    ]
    for i in range(5):
        loads[i].start()
    for mask_load in masks:
        mask_load.start()
    for i in range(5, len(loads)):
        loads[i].start()

    step_rows = rows // CHUNKS

    def chunk(c):
        return pl.ds(c * step_rows, step_rows)

    def copy(source, target, span, send, receive, device):
        return pltpu.make_async_remote_copy(
            src_ref=slab_ref.at[source, span], dst_ref=slab_ref.at[target, span],
            send_sem=send, recv_sem=receive,
            device_id={"blk": device}, device_id_type=MESH,
        )

    def partner_copy():
        return copy(OWN, PARTNER, pl.ds(0, rows), p_send, p_recv, partner)

    def mirror_copy(c):
        return copy(OWN, MIRROR, chunk(c), m_send, recv.at[0, c], mirror)

    def rail_copy(c):
        return copy(MIRROR, RAIL, chunk(c), r_send, recv.at[1, c], rail_to)

    def cross_copy(c, source):
        return copy(source, CROSS, chunk(c), c_send, recv.at[2, c], partner)

    def sent():
        for source, target, send, device in (
            (OWN, PARTNER, p_send, partner), (OWN, MIRROR, m_send, mirror),
            (MIRROR, RAIL, r_send, rail_to), (RAIL, CROSS, c_send, partner),
        ):
            copy(source, target, pl.ds(0, rows), send, p_recv, device).wait_send()

    def got_mirror(c):
        mirror_copy(c).wait_recv()
        rail_copy(c).start()

        @pl.when(same)
        def _():
            cross_copy(c, MIRROR).start()

    def got_rail(c):
        rail_copy(c).wait_recv()

        @pl.when(jnp.logical_not(same))
        def _():
            cross_copy(c, RAIL).start()

    def got_cross(c):
        cross_copy(c, RAIL).wait_recv()

    loads[0].wait()
    pl.semaphore_wait(
        barrier, 3 + (group > 0).astype(jnp.int32) + (group < groups - 1).astype(jnp.int32)
    )
    for c in range(CHUNKS):
        mirror_copy(c).start()
    partner_copy().start()
    roll_call_start()

    def normalize(value):
        full = value.astype(jnp.float32)
        return (
            full * lax.rsqrt(jnp.mean(full * full, axis=-1, keepdims=True) + 1e-06) * ng_ref[0:1]
        ).astype(jnp.bfloat16)

    def unit(pieces, count):
        total = len(pieces) * count
        for i, (slot, start) in enumerate(pieces):
            normed_ref[i * count:(i + 1) * count] = normalize(
                slab_ref[slot, pl.ds(start, count), :]
            )
        kb_ref[...] = jnp.dot(
            normed_ref[...], wk_ref[...], preferred_element_type=jnp.float32
        ).astype(jnp.bfloat16)
        values = lax.dot_general(
            wvt_ref[...], normed_ref[...], (((1,), (1,)), ((), ())),
            preferred_element_type=jnp.float32,
        ).astype(jnp.bfloat16)
        for h in range(heads):
            vt_ref[h, :HEAD_DIM] = values[h * HEAD_DIM:(h + 1) * HEAD_DIM]
        atom = lax.broadcasted_iota(jnp.int32, (rows, PAIR), 0)
        other = lax.broadcasted_iota(jnp.int32, (rows, PAIR), 1)
        for i, (slot, start) in enumerate(pieces):
            linked = mask_ref[slot, :, pl.ds(pl.multiple_of(start, PAIR), PAIR)] > 0
            shift = start + jnp.where(slot == OWN, 0, rows)
            bias_ref[i * count:(i + 1) * count, :] = jnp.where(
                linked | (atom == other + shift), 0.0, NEG
            ).T

        def scores(h):
            pair = h // 2
            piece = kb_ref[:total, pair * PAIR:(pair + 1) * PAIR]
            score = jnp.dot(
                jnp.concatenate([piece, piece], axis=1), qt_ref[h],
                preferred_element_type=jnp.float32,
            ) + bias_ref[:total]
            s_ref[h % SLOTS, :total] = score
            return jnp.max(score, axis=0, keepdims=True)

        def finish(h, peak):
            old = m_ref[h, 0:1]
            new = jnp.maximum(old, peak)
            m_ref[h, 0:1] = new
            weight = jnp.exp2(s_ref[h % SLOTS, :total] - new).astype(jnp.bfloat16)
            result = jnp.dot(vt_ref[h, :, :total], weight, preferred_element_type=jnp.float32)
            acc_ref[h] = acc_ref[h] * jnp.exp2(old - new) + result

        peaks = [scores(h) for h in range(LOOK)]
        for h in range(heads):
            if h + LOOK < heads:
                peaks.append(scores(h + LOOK))
            finish(h, peaks[h])

    ones = jnp.ones((heads, SUMS, vt_ref.shape[2]), jnp.bfloat16)
    vt_ref[:, HEAD_DIM:, :] = ones
    m_ref[...] = jnp.full(m_ref.shape, NEG, jnp.float32)
    acc_ref[...] = jnp.zeros(acc_ref.shape, jnp.float32)

    loads[1].wait()
    normed = normalize(slab_ref[OWN])
    loads[2].wait()
    wqt = wq_ref[...].T
    query = lax.dot_general(
        wqt, normed, (((1,), (1,)), ((), ())), preferred_element_type=jnp.float32
    ).astype(jnp.bfloat16).astype(jnp.float32) * SCALE
    high = query.astype(jnp.bfloat16)
    low = (query - high.astype(jnp.float32)).astype(jnp.bfloat16)
    zero = jnp.zeros((HEAD_DIM, rows), jnp.bfloat16)
    for h in range(heads):
        span = slice(h * HEAD_DIM, (h + 1) * HEAD_DIM)
        for part, base in ((high, 0), (low, PAIR)):
            here = base + (h % 2) * HEAD_DIM
            there = base + (1 - h % 2) * HEAD_DIM
            qt_ref[h, here:here + HEAD_DIM] = part[span]
            qt_ref[h, there:there + HEAD_DIM] = zero
    roll_call_early()
    loads[4].wait()
    wvt_ref[...] = wv_ref[...].T
    loads[3].wait()

    actions = {
        "p": lambda c: partner_copy().wait_recv(),
        "e": lambda c: roll_call_end(),
        "m": got_mirror, "r": got_rail,
        "c": got_cross,
    }

    def run(listed):
        for kind, low_c, high_c in listed:
            for c in range(low_c, high_c):
                actions[kind](c)

    def run_events(u, table):
        for k, listed in table.items():
            @pl.when(u == k)
            def _():
                run(listed)

    half = rows // 2

    def step(u, carry):
        run_events(u, {
            1: (("e", 0, 1), ("m", 0, 1)),
            2: (("p", 0, 1), ("m", 1, 2)),
            3: (("m", 2, 3),),
            4: (("m", 3, 5),),
            5: (("r", 0, 1), ("m", 5, 6), ("r", 1, 2), ("c", 0, 2), ("r", 2, 3), ("m", 6, 7)),
            6: (("r", 3, 4), ("m", 7, 8)),
            7: (("r", 4, 5), ("c", 2, 4)),
            8: (("r", 5, 6), ("c", 4, 6)),
            9: (("r", 6, 8), ("c", 6, 8)),
        })
        for k, listed in ((0, (0,)), (2, (1,)), (4, (2,)), (5, (3, 4))):
            @pl.when(u == k)
            def _():
                for i in listed:
                    masks[i].wait()
        plain = (u < 5) | (u == 6)
        slot = jnp.where(u < 4, u // 2, jnp.where(plain, MIRROR, RAIL))
        start = jnp.where(
            u < 4, (u % 2) * half,
            jnp.where(
                plain, (u // 6) * half,
                jnp.where(u == 5, 0, (u - 6) * PAIR),
            ),
        )
        slot_too = jnp.where(plain, slot, CROSS)
        start_too = jnp.where(plain, start + PAIR, start)
        unit([(slot, start), (slot_too, start_too)], PAIR)
        return carry

    lax.fori_loop(0, 5, step, 0)
    lax.fori_loop(5, 10, step, 0)

    for h in range(heads):
        inverse = 1.0 / acc_ref[h, HEAD_DIM:HEAD_DIM + 1]
        mixed_ref[h * HEAD_DIM:(h + 1) * HEAD_DIM, :] = (
            acc_ref[h, :HEAD_DIM] * inverse
        ).astype(jnp.bfloat16)
    for load in loads[5:]:
        load.wait()
    after_ref[...] = slab_ref[OWN].astype(jnp.float32) + jnp.dot(
        mixed_ref[...].T, wo_ref[...], preferred_element_type=jnp.float32
    )

    local_mean = jnp.sum(after_ref[...], axis=0, keepdims=True) * (1.0 / rows)
    spread = after_ref[...] - local_mean
    stats_ref[0, 0:1] = local_mean
    stats_ref[0, 1:2] = jnp.sum(spread * spread, axis=0, keepdims=True)

    def stats_copy(source, target, device):
        return pltpu.make_async_remote_copy(
            src_ref=stats_ref.at[source], dst_ref=stats_ref.at[target],
            send_sem=s_send, recv_sem=s_recv,
            device_id={"blk": device}, device_id_type=MESH,
        )

    def send_stats(d, carry):
        stats_copy(0, d, lax.rem(me + d, n)).start()
        return carry

    lax.fori_loop(1, n, send_stats, 0)
    sent()
    others = pl.ds(1, n - 1)
    stats_copy(others, others, partner).wait_recv()
    gathered = stats_ref[...]
    means = gathered[:, 0, :]
    mean = jnp.sum(means, axis=0, keepdims=True) * (1.0 / n)
    shifts = means - mean
    var = (
        jnp.sum(gathered[:, 1, :], axis=0, keepdims=True) * (1.0 / rows)
        + jnp.sum(shifts * shifts, axis=0, keepdims=True)
    ) * (1.0 / n)
    gain = lax.rsqrt(var + 1e-05) * bg_ref[0:1]
    batched = ((after_ref[...] - mean) * gain + bs_ref[0:1]).astype(jnp.bfloat16)
    hidden = jax.nn.gelu(
        jnp.dot(batched, wu_ref[...], preferred_element_type=jnp.float32), approximate=True
    ).astype(jnp.bfloat16)
    out_ref[...] = (
        after_ref[...] + jnp.dot(hidden, wd_ref[...], preferred_element_type=jnp.float32)
    ).astype(jnp.bfloat16)

    stats_copy(others, others, partner).wait_send()


def body(
    atoms, edge_mask, norm_gain, w_query, w_key, w_value, w_out, bn_gain, bn_shift, w_up, w_down
):
    n = lax.axis_size("blk")
    rows, width = atoms.shape
    ff = w_up.shape[1]
    slabs = edge_mask.shape[1]
    heads = width // HEAD_DIM
    bf16, f32 = jnp.bfloat16, jnp.float32
    dma = pltpu.SemaphoreType.DMA
    return pl.pallas_call(
        functools.partial(kernel, n),
        out_shape=pltpu.VMEM((rows, width), bf16),
        in_specs=[pl.BlockSpec(memory_space=pl.ANY)] * 11,
        out_specs=pl.BlockSpec(memory_space=pltpu.VMEM),
        scratch_shapes=[
            pltpu.VMEM((slabs, rows, width), bf16),
            pltpu.VMEM((slabs, rows, rows), jnp.int32),
            pltpu.VMEM((8, width), f32),
            pltpu.VMEM((width, width), bf16),
            pltpu.VMEM((width, width), bf16),
            pltpu.VMEM((width, width), bf16),
            pltpu.VMEM((width, width), bf16),
            pltpu.VMEM((8, width), f32),
            pltpu.VMEM((8, width), f32),
            pltpu.VMEM((width, ff), bf16),
            pltpu.VMEM((ff, width), bf16),
            pltpu.VMEM((width, width), bf16),
            pltpu.VMEM((heads, 2 * PAIR, rows), bf16),
            pltpu.VMEM((2 * PAIR, width), bf16),
            pltpu.VMEM((2 * PAIR, width), bf16),
            pltpu.VMEM((heads, HEAD_DIM + SUMS, 2 * PAIR), bf16),
            pltpu.VMEM((2 * PAIR, rows), f32),
            pltpu.VMEM((heads, 8, rows), f32),
            pltpu.VMEM((SLOTS, 2 * PAIR, rows), f32),
            pltpu.VMEM((heads, HEAD_DIM + SUMS, rows), f32),
            pltpu.VMEM((width, rows), bf16),
            pltpu.VMEM((rows, width), f32),
            pltpu.VMEM((n, 2, width), f32),
            dma((10,)),
            dma((slabs,)),
            dma, dma, dma, dma, dma,
            dma((3, CHUNKS)),
            dma, dma,
            pltpu.SemaphoreType.REGULAR, pltpu.SemaphoreType.REGULAR,
        ],
        compiler_params=pltpu.CompilerParams(
            collective_id=0, has_side_effects=True, vmem_limit_bytes=60 * 1024 * 1024
        ),
    )(
        atoms, edge_mask, norm_gain.reshape(1, width), w_query, w_key, w_value, w_out,
        bn_gain.reshape(1, width), bn_shift.reshape(1, width), w_up, w_down,
    )


def solution(mesh):
    placed = (
        P(("grp", "blk"), None),
        P(("grp", "blk"), None, None, None),
        P(), P(), P(), P(), P(), P(), P(), P(), P(),
    )
    return jax.shard_map(
        body, mesh=mesh, in_specs=placed, out_specs=P(("grp", "blk"), None), check_vma=False
    )
```

```python
import functools
import math

import jax
import jax.numpy as jnp
from jax import lax
from jax.experimental import pallas as pl
from jax.experimental.pallas import tpu as pltpu
from jax.sharding import PartitionSpec as P

HEAD_DIM = 64
PAIR = 2 * HEAD_DIM
REACH = 2
CHUNKS = 8
SUMS = 16
LOOK = 3
SLOTS = LOOK + 1
NEG = -1e30
MESH = pl.DeviceIdType.MESH
OWN, PARTNER, MIRROR, RAIL, CROSS = 0, 1, 2, 3, 4
SCALE = math.log2(math.e) * HEAD_DIM ** (-0.5)


def kernel(
    n,
    atoms_hbm, mask_hbm, ng_hbm, wq_hbm, wk_hbm, wv_hbm, wo_hbm, bg_hbm, bs_hbm, wu_hbm, wd_hbm,
    out_ref,
    x_ref, slab_ref, mask_ref, ng_ref, wq_ref, wk_ref, wv_ref, wo_ref, bg_ref, bs_ref, wu_ref, wd_ref,
    wvt_ref, qt_ref, kb_ref, vt_ref, bias_ref, m_ref, s_ref, acc_ref, mixed_ref, after_ref,
    stats_ref, load_sem, mask_sem,
    p_send, p_recv, m_send, r_send, c_send, recv, s_send, s_recv, up_sem, down_sem,
):
    me = lax.axis_index("blk")
    rows, width = after_ref.shape
    heads = width // HEAD_DIM
    group, inside = me // 4, me % 4
    side, core = inside // 2, inside % 2
    cousin = group * 4 + (1 - side) * 2 + (1 - core)
    partner = group * 4 + side * 2 + (1 - core)
    mirror = group * 4 + (1 - side) * 2 + core
    groups = n // 4
    rail_to = ((group + 1 - 2 * side + groups) % groups) * 4 + side * 2 + core
    same = side == core

    barrier = pltpu.get_barrier_semaphore()

    for known in (partner, mirror, cousin):
        pl.semaphore_signal(barrier, inc=1, device_id={"blk": known}, device_id_type=MESH)

    @pl.when(group > 0)
    def _():
        pl.semaphore_signal(barrier, inc=1, device_id={"blk": me - 4}, device_id_type=MESH)

    @pl.when(group < groups - 1)
    def _():
        pl.semaphore_signal(barrier, inc=1, device_id={"blk": me + 4}, device_id_type=MESH)

    def tell_up():
        @pl.when(group < groups - 1)
        def _():
            pl.semaphore_signal(up_sem, inc=1, device_id={"blk": me + 4}, device_id_type=MESH)

    def tell_down():
        @pl.when(group > 0)
        def _():
            pl.semaphore_signal(down_sem, inc=1, device_id={"blk": me - 4}, device_id_type=MESH)

    def roll_call_start():
        @pl.when(group == 0)
        def _():
            tell_up()

        @pl.when(group == groups - 1)
        def _():
            tell_down()

    def roll_call_early():
        @pl.when(group == 1)
        def _():
            pl.semaphore_wait(up_sem, 1)
            tell_up()

        @pl.when(group == groups - 2)
        def _():
            pl.semaphore_wait(down_sem, 1)
            tell_down()

    def roll_call_end():
        @pl.when(group > 1)
        def _():
            pl.semaphore_wait(up_sem, 1)
            tell_up()

        @pl.when(group < groups - 2)
        def _():
            pl.semaphore_wait(down_sem, 1)
            tell_down()

    sources = (
        (atoms_hbm, x_ref), (ng_hbm, ng_ref.at[0:1]), (wq_hbm, wq_ref), (wk_hbm, wk_ref),
        (wv_hbm, wv_ref), (wo_hbm, wo_ref), (bg_hbm, bg_ref.at[0:1]), (bs_hbm, bs_ref.at[0:1]),
        (wu_hbm, wu_ref), (wd_hbm, wd_ref),
    )
    loads = [
        pltpu.make_async_copy(src, dst, load_sem.at[i]) for i, (src, dst) in enumerate(sources)
    ]
    far = jnp.where(side == 0, 2, -2)
    near = jnp.where(core == 0, 1, -1)
    offsets = [jnp.int32(0), near, far, -far, -near]
    masks = [
        pltpu.make_async_copy(
            mask_hbm.at[0, offsets[i] + REACH], mask_ref.at[i], mask_sem.at[i]
        )
        for i in range(2 * REACH + 1)
    ]
    for i in range(5):
        loads[i].start()
    for mask_load in masks:
        mask_load.start()
    for i in range(5, len(loads)):
        loads[i].start()

    step_rows = rows // CHUNKS

    def chunk(c):
        return pl.ds(c * step_rows, step_rows)

    def copy(source, target, span, send, receive, device):
        return pltpu.make_async_remote_copy(
            src_ref=slab_ref.at[source, span], dst_ref=slab_ref.at[target, span],
            send_sem=send, recv_sem=receive,
            device_id={"blk": device}, device_id_type=MESH,
        )

    def partner_copy():
        return copy(OWN, PARTNER, pl.ds(0, rows), p_send, p_recv, partner)

    def mirror_copy(c):
        return copy(OWN, MIRROR, chunk(c), m_send, recv.at[0, c], mirror)

    def rail_copy(c):
        return copy(MIRROR, RAIL, chunk(c), r_send, recv.at[1, c], rail_to)

    def cross_copy(c, source):
        return copy(source, CROSS, chunk(c), c_send, recv.at[2, c], partner)

    def sent():
        for source, target, send, device in (
            (OWN, PARTNER, p_send, partner), (OWN, MIRROR, m_send, mirror),
            (MIRROR, RAIL, r_send, rail_to), (RAIL, CROSS, c_send, partner),
        ):
            copy(source, target, pl.ds(0, rows), send, p_recv, device).wait_send()

    def got_mirror(c):
        mirror_copy(c).wait_recv()
        rail_copy(c).start()

        @pl.when(same)
        def _():
            cross_copy(c, MIRROR).start()

    def got_rail(c):
        rail_copy(c).wait_recv()

        @pl.when(jnp.logical_not(same))
        def _():
            cross_copy(c, RAIL).start()

    def got_cross(c):
        cross_copy(c, RAIL).wait_recv()

    def normalize(value):
        full = value.astype(jnp.float32)
        return (
            full * lax.rsqrt(jnp.mean(full * full, axis=-1, keepdims=True) + 1e-06) * ng_ref[0:1]
        ).astype(jnp.bfloat16)

    loads[0].wait()
    loads[1].wait()
    slab_ref[OWN] = normalize(x_ref[...])
    pl.semaphore_wait(
        barrier, 3 + (group > 0).astype(jnp.int32) + (group < groups - 1).astype(jnp.int32)
    )
    for c in range(CHUNKS):
        mirror_copy(c).start()
    partner_copy().start()
    roll_call_start()

    def unit(pieces, count):
        total = len(pieces) * count
        normed = jnp.concatenate(
            [slab_ref[slot, pl.ds(start, count), :] for slot, start in pieces], axis=0
        )
        kb_ref[...] = jnp.dot(
            normed, wk_ref[...], preferred_element_type=jnp.float32
        ).astype(jnp.bfloat16)
        values = lax.dot_general(
            wvt_ref[...], normed, (((1,), (1,)), ((), ())),
            preferred_element_type=jnp.float32,
        ).astype(jnp.bfloat16)
        for h in range(heads):
            vt_ref[h, :HEAD_DIM] = values[h * HEAD_DIM:(h + 1) * HEAD_DIM]
        atom = lax.broadcasted_iota(jnp.int32, (rows, PAIR), 0)
        other = lax.broadcasted_iota(jnp.int32, (rows, PAIR), 1)
        for i, (slot, start) in enumerate(pieces):
            linked = mask_ref[slot, :, pl.ds(pl.multiple_of(start, PAIR), PAIR)] > 0
            shift = start + jnp.where(slot == OWN, 0, rows)
            bias_ref[i * count:(i + 1) * count, :] = jnp.where(
                linked | (atom == other + shift), 0.0, NEG
            ).T

        def scores(h):
            pair = h // 2
            piece = kb_ref[:total, pair * PAIR:(pair + 1) * PAIR]
            score = jnp.dot(
                jnp.concatenate([piece, piece], axis=1), qt_ref[h],
                preferred_element_type=jnp.float32,
            ) + bias_ref[:total]
            s_ref[h % SLOTS, :total] = score
            return jnp.max(score, axis=0, keepdims=True)

        def finish(h, peak):
            old = m_ref[h, 0:1]
            new = jnp.maximum(old, peak)
            m_ref[h, 0:1] = new
            weight = jnp.exp2(s_ref[h % SLOTS, :total] - new).astype(jnp.bfloat16)
            result = jnp.dot(vt_ref[h, :, :total], weight, preferred_element_type=jnp.float32)
            acc_ref[h] = acc_ref[h] * jnp.exp2(old - new) + result

        peaks = [scores(h) for h in range(LOOK)]
        for h in range(heads):
            if h + LOOK < heads:
                peaks.append(scores(h + LOOK))
            finish(h, peaks[h])

    ones = jnp.ones((heads, SUMS, vt_ref.shape[2]), jnp.bfloat16)
    vt_ref[:, HEAD_DIM:, :] = ones
    m_ref[...] = jnp.full(m_ref.shape, NEG, jnp.float32)
    acc_ref[...] = jnp.zeros(acc_ref.shape, jnp.float32)

    normed = slab_ref[OWN]
    loads[2].wait()
    wqt = wq_ref[...].T
    query = lax.dot_general(
        wqt, normed, (((1,), (1,)), ((), ())), preferred_element_type=jnp.float32
    ).astype(jnp.bfloat16).astype(jnp.float32) * SCALE
    high = query.astype(jnp.bfloat16)
    low = (query - high.astype(jnp.float32)).astype(jnp.bfloat16)
    zero = jnp.zeros((HEAD_DIM, rows), jnp.bfloat16)
    for h in range(heads):
        span = slice(h * HEAD_DIM, (h + 1) * HEAD_DIM)
        for part, base in ((high, 0), (low, PAIR)):
            here = base + (h % 2) * HEAD_DIM
            there = base + (1 - h % 2) * HEAD_DIM
            qt_ref[h, here:here + HEAD_DIM] = part[span]
            qt_ref[h, there:there + HEAD_DIM] = zero
    roll_call_early()
    loads[4].wait()
    wvt_ref[...] = wv_ref[...].T
    loads[3].wait()

    actions = {
        "p": lambda c: partner_copy().wait_recv(),
        "e": lambda c: roll_call_end(),
        "m": got_mirror, "r": got_rail,
        "c": got_cross,
    }

    def run(listed):
        for kind, low_c, high_c in listed:
            for c in range(low_c, high_c):
                actions[kind](c)

    def run_events(u, table):
        for k, listed in table.items():
            @pl.when(u == k)
            def _():
                run(listed)

    half = rows // 2

    def step(u, carry):
        run_events(u, {
            1: (("e", 0, 1), ("m", 0, 1)),
            2: (("p", 0, 1), ("m", 1, 2)),
            3: (("m", 2, 4),),
            4: (("m", 4, 5),),
            5: (("r", 0, 1), ("m", 5, 6), ("r", 1, 2), ("c", 0, 2)),
            6: (("m", 6, 7), ("r", 2, 4), ("m", 7, 8)),
            7: (("r", 4, 5), ("c", 2, 4)),
            8: (("r", 5, 6), ("c", 4, 6)),
            9: (("r", 6, 8), ("c", 6, 8)),
        })
        for k, listed in ((0, (0,)), (2, (1,)), (3, (2,)), (5, (3, 4))):
            @pl.when(u == k)
            def _():
                for i in listed:
                    masks[i].wait()
        plain = (u < 5) | (u == 6)
        slot = jnp.where(
            u < 3, u // 2,
            jnp.where(u == 4, PARTNER, jnp.where(plain, MIRROR, RAIL)),
        )
        start = jnp.where(
            u < 3, (u % 2) * half,
            jnp.where(
                plain, jnp.where(u == 3, 0, half),
                jnp.where(u == 5, 0, (u - 6) * PAIR),
            ),
        )
        slot_too = jnp.where(plain, slot, CROSS)
        start_too = jnp.where(plain, start + PAIR, start)
        unit([(slot, start), (slot_too, start_too)], PAIR)
        return carry

    lax.fori_loop(0, 5, step, 0)
    lax.fori_loop(5, 10, step, 0)

    for h in range(heads):
        inverse = 1.0 / acc_ref[h, HEAD_DIM:HEAD_DIM + 1]
        mixed_ref[h * HEAD_DIM:(h + 1) * HEAD_DIM, :] = (
            acc_ref[h, :HEAD_DIM] * inverse
        ).astype(jnp.bfloat16)
    for load in loads[5:]:
        load.wait()
    after_ref[...] = x_ref[...].astype(jnp.float32) + jnp.dot(
        mixed_ref[...].T, wo_ref[...], preferred_element_type=jnp.float32
    )

    local_mean = jnp.sum(after_ref[...], axis=0, keepdims=True) * (1.0 / rows)
    spread = after_ref[...] - local_mean
    stats_ref[0, 0:1] = local_mean
    stats_ref[0, 1:2] = jnp.sum(spread * spread, axis=0, keepdims=True)

    def stats_copy(source, target, device):
        return pltpu.make_async_remote_copy(
            src_ref=stats_ref.at[source], dst_ref=stats_ref.at[target],
            send_sem=s_send, recv_sem=s_recv,
            device_id={"blk": device}, device_id_type=MESH,
        )

    def send_stats(d, carry):
        stats_copy(0, d, lax.rem(me + d, n)).start()
        return carry

    lax.fori_loop(1, n, send_stats, 0)
    sent()
    others = pl.ds(1, n - 1)
    stats_copy(others, others, partner).wait_recv()
    gathered = stats_ref[...]
    means = gathered[:, 0, :]
    mean = jnp.sum(means, axis=0, keepdims=True) * (1.0 / n)
    shifts = means - mean
    var = (
        jnp.sum(gathered[:, 1, :], axis=0, keepdims=True) * (1.0 / rows)
        + jnp.sum(shifts * shifts, axis=0, keepdims=True)
    ) * (1.0 / n)
    gain = lax.rsqrt(var + 1e-05) * bg_ref[0:1]
    batched = ((after_ref[...] - mean) * gain + bs_ref[0:1]).astype(jnp.bfloat16)
    hidden = jax.nn.gelu(
        jnp.dot(batched, wu_ref[...], preferred_element_type=jnp.float32), approximate=True
    ).astype(jnp.bfloat16)
    out_ref[...] = (
        after_ref[...] + jnp.dot(hidden, wd_ref[...], preferred_element_type=jnp.float32)
    ).astype(jnp.bfloat16)

    stats_copy(others, others, partner).wait_send()


def body(
    atoms, edge_mask, norm_gain, w_query, w_key, w_value, w_out, bn_gain, bn_shift, w_up, w_down
):
    n = lax.axis_size("blk")
    rows, width = atoms.shape
    ff = w_up.shape[1]
    slabs = edge_mask.shape[1]
    heads = width // HEAD_DIM
    bf16, f32 = jnp.bfloat16, jnp.float32
    dma = pltpu.SemaphoreType.DMA
    return pl.pallas_call(
        functools.partial(kernel, n),
        out_shape=pltpu.VMEM((rows, width), bf16),
        in_specs=[pl.BlockSpec(memory_space=pl.ANY)] * 11,
        out_specs=pl.BlockSpec(memory_space=pltpu.VMEM),
        scratch_shapes=[
            pltpu.VMEM((rows, width), bf16),
            pltpu.VMEM((slabs, rows, width), bf16),
            pltpu.VMEM((slabs, rows, rows), jnp.int32),
            pltpu.VMEM((8, width), f32),
            pltpu.VMEM((width, width), bf16),
            pltpu.VMEM((width, width), bf16),
            pltpu.VMEM((width, width), bf16),
            pltpu.VMEM((width, width), bf16),
            pltpu.VMEM((8, width), f32),
            pltpu.VMEM((8, width), f32),
            pltpu.VMEM((width, ff), bf16),
            pltpu.VMEM((ff, width), bf16),
            pltpu.VMEM((width, width), bf16),
            pltpu.VMEM((heads, 2 * PAIR, rows), bf16),
            pltpu.VMEM((2 * PAIR, width), bf16),
            pltpu.VMEM((heads, HEAD_DIM + SUMS, 2 * PAIR), bf16),
            pltpu.VMEM((2 * PAIR, rows), f32),
            pltpu.VMEM((heads, 8, rows), f32),
            pltpu.VMEM((SLOTS, 2 * PAIR, rows), f32),
            pltpu.VMEM((heads, HEAD_DIM + SUMS, rows), f32),
            pltpu.VMEM((width, rows), bf16),
            pltpu.VMEM((rows, width), f32),
            pltpu.VMEM((n, 2, width), f32),
            dma((10,)),
            dma((slabs,)),
            dma, dma, dma, dma, dma,
            dma((3, CHUNKS)),
            dma, dma,
            pltpu.SemaphoreType.REGULAR, pltpu.SemaphoreType.REGULAR,
        ],
        compiler_params=pltpu.CompilerParams(
            collective_id=0, has_side_effects=True, vmem_limit_bytes=60 * 1024 * 1024
        ),
    )(
        atoms, edge_mask, norm_gain.reshape(1, width), w_query, w_key, w_value, w_out,
        bn_gain.reshape(1, width), bn_shift.reshape(1, width), w_up, w_down,
    )


def solution(mesh):
    placed = (
        P(("grp", "blk"), None),
        P(("grp", "blk"), None, None, None),
        P(), P(), P(), P(), P(), P(), P(), P(), P(),
    )
    return jax.shard_map(
        body, mesh=mesh, in_specs=placed, out_specs=P(("grp", "blk"), None), check_vma=False
    )
```

```python
import functools
import math

import jax
import jax.numpy as jnp
from jax import lax
from jax.experimental import pallas as pl
from jax.experimental.pallas import tpu as pltpu
from jax.sharding import PartitionSpec as P

HEAD_DIM = 64
PAIR = 2 * HEAD_DIM
REACH = 2
CHUNKS = 8
SUMS = 16
LOOK = 3
SLOTS = LOOK + 1
NEG = -1e30
MESH = pl.DeviceIdType.MESH
OWN, PARTNER, MIRROR, RAIL, CROSS = 0, 1, 2, 3, 4
SCALE = math.log2(math.e) * HEAD_DIM ** (-0.5)


def kernel(
    n,
    atoms_hbm, mask_hbm, ng_hbm, wq_hbm, wk_hbm, wv_hbm, wo_hbm, bg_hbm, bs_hbm, wu_hbm, wd_hbm,
    out_ref,
    x_ref, slab_ref, mask_ref, ng_ref, wq_ref, wk_ref, wv_ref, wo_ref, bg_ref, bs_ref, wu_ref, wd_ref,
    wvt_ref, qt_ref, kb_ref, vt_ref, bias_ref, m_ref, s_ref, acc_ref, mixed_ref, after_ref,
    stats_ref, load_sem, mask_sem,
    p_send, p_recv, m_send, r_send, c_send, recv, s_send, s_recv, up_sem, down_sem,
):
    me = lax.axis_index("blk")
    rows, width = after_ref.shape
    heads = width // HEAD_DIM
    group, inside = me // 4, me % 4
    side, core = inside // 2, inside % 2
    cousin = group * 4 + (1 - side) * 2 + (1 - core)
    partner = group * 4 + side * 2 + (1 - core)
    mirror = group * 4 + (1 - side) * 2 + core
    groups = n // 4
    rail_to = ((group + 1 - 2 * side + groups) % groups) * 4 + side * 2 + core
    same = side == core

    barrier = pltpu.get_barrier_semaphore()

    for known in (partner, mirror, cousin):
        pl.semaphore_signal(barrier, inc=1, device_id={"blk": known}, device_id_type=MESH)

    @pl.when(group > 0)
    def _():
        pl.semaphore_signal(barrier, inc=1, device_id={"blk": me - 4}, device_id_type=MESH)

    @pl.when(group < groups - 1)
    def _():
        pl.semaphore_signal(barrier, inc=1, device_id={"blk": me + 4}, device_id_type=MESH)

    def tell_up():
        @pl.when(group < groups - 1)
        def _():
            pl.semaphore_signal(up_sem, inc=1, device_id={"blk": me + 4}, device_id_type=MESH)

    def tell_down():
        @pl.when(group > 0)
        def _():
            pl.semaphore_signal(down_sem, inc=1, device_id={"blk": me - 4}, device_id_type=MESH)

    def roll_call_start():
        @pl.when(group == 0)
        def _():
            tell_up()

        @pl.when(group == groups - 1)
        def _():
            tell_down()

    def roll_call_early():
        @pl.when(group == 1)
        def _():
            pl.semaphore_wait(up_sem, 1)
            tell_up()

        @pl.when(group == groups - 2)
        def _():
            pl.semaphore_wait(down_sem, 1)
            tell_down()

    def roll_call_end():
        @pl.when(group > 1)
        def _():
            pl.semaphore_wait(up_sem, 1)
            tell_up()

        @pl.when(group < groups - 2)
        def _():
            pl.semaphore_wait(down_sem, 1)
            tell_down()

    sources = (
        (atoms_hbm, x_ref), (ng_hbm, ng_ref.at[0:1]), (wq_hbm, wq_ref), (wk_hbm, wk_ref),
        (wv_hbm, wv_ref), (wo_hbm, wo_ref), (bg_hbm, bg_ref.at[0:1]), (bs_hbm, bs_ref.at[0:1]),
        (wu_hbm, wu_ref), (wd_hbm, wd_ref),
    )
    loads = [
        pltpu.make_async_copy(src, dst, load_sem.at[i]) for i, (src, dst) in enumerate(sources)
    ]
    far = jnp.where(side == 0, 2, -2)
    near = jnp.where(core == 0, 1, -1)
    offsets = [jnp.int32(0), near, far, -far, -near]
    masks = [
        pltpu.make_async_copy(
            mask_hbm.at[0, offsets[i] + REACH], mask_ref.at[i], mask_sem.at[i]
        )
        for i in range(2 * REACH + 1)
    ]
    for i in range(5):
        loads[i].start()
    for mask_load in masks:
        mask_load.start()
    for i in range(5, len(loads)):
        loads[i].start()

    step_rows = rows // CHUNKS

    def chunk(c):
        return pl.ds(c * step_rows, step_rows)

    def copy(source, target, span, send, receive, device):
        return pltpu.make_async_remote_copy(
            src_ref=slab_ref.at[source, span], dst_ref=slab_ref.at[target, span],
            send_sem=send, recv_sem=receive,
            device_id={"blk": device}, device_id_type=MESH,
        )

    def partner_copy():
        return copy(OWN, PARTNER, pl.ds(0, rows), p_send, p_recv, partner)

    def mirror_copy(c):
        return copy(OWN, MIRROR, chunk(c), m_send, recv.at[0, c], mirror)

    def rail_copy(c):
        return copy(MIRROR, RAIL, chunk(c), r_send, recv.at[1, c], rail_to)

    def cross_copy(c, source):
        return copy(source, CROSS, chunk(c), c_send, recv.at[2, c], partner)

    def sent():
        for source, target, send, device in (
            (OWN, PARTNER, p_send, partner), (OWN, MIRROR, m_send, mirror),
            (MIRROR, RAIL, r_send, rail_to), (RAIL, CROSS, c_send, partner),
        ):
            copy(source, target, pl.ds(0, rows), send, p_recv, device).wait_send()

    def got_mirror(c):
        mirror_copy(c).wait_recv()
        rail_copy(c).start()

        @pl.when(same)
        def _():
            cross_copy(c, MIRROR).start()

    def got_rail(c):
        rail_copy(c).wait_recv()

        @pl.when(jnp.logical_not(same))
        def _():
            cross_copy(c, RAIL).start()

    def got_cross(c):
        cross_copy(c, RAIL).wait_recv()

    def normalize(value):
        full = value.astype(jnp.float32)
        return (
            full * lax.rsqrt(jnp.mean(full * full, axis=-1, keepdims=True) + 1e-06) * ng_ref[0:1]
        ).astype(jnp.bfloat16)

    loads[0].wait()
    loads[1].wait()
    slab_ref[OWN] = normalize(x_ref[...])
    pl.semaphore_wait(
        barrier, 3 + (group > 0).astype(jnp.int32) + (group < groups - 1).astype(jnp.int32)
    )
    for c in range(CHUNKS):
        mirror_copy(c).start()
    partner_copy().start()
    roll_call_start()

    def unit(pieces, count):
        total = len(pieces) * count
        normed = jnp.concatenate(
            [slab_ref[slot, pl.ds(start, count), :] for slot, start in pieces], axis=0
        )
        kb_ref[...] = jnp.dot(
            normed, wk_ref[...], preferred_element_type=jnp.float32
        ).astype(jnp.bfloat16)
        values = lax.dot_general(
            wvt_ref[...], normed, (((1,), (1,)), ((), ())),
            preferred_element_type=jnp.float32,
        ).astype(jnp.bfloat16)
        for h in range(heads):
            vt_ref[h, :HEAD_DIM] = values[h * HEAD_DIM:(h + 1) * HEAD_DIM]
        atom = lax.broadcasted_iota(jnp.int32, (rows, PAIR), 0)
        other = lax.broadcasted_iota(jnp.int32, (rows, PAIR), 1)
        for i, (slot, start) in enumerate(pieces):
            linked = mask_ref[slot, :, pl.ds(pl.multiple_of(start, PAIR), PAIR)] > 0
            shift = start + jnp.where(slot == OWN, 0, rows)
            bias_ref[i * count:(i + 1) * count, :] = jnp.where(
                linked | (atom == other + shift), 0.0, NEG
            ).T

        def scores(h):
            pair = h // 2
            piece = kb_ref[:total, pair * PAIR:(pair + 1) * PAIR]
            score = jnp.dot(
                jnp.concatenate([piece, piece], axis=1), qt_ref[h],
                preferred_element_type=jnp.float32,
            ) + bias_ref[:total]
            s_ref[h % SLOTS, :total] = score
            return jnp.max(score, axis=0, keepdims=True)

        def finish(h, peak):
            old = m_ref[h, 0:1]
            new = jnp.maximum(old, peak)
            m_ref[h, 0:1] = new
            weight = jnp.exp2(s_ref[h % SLOTS, :total] - new).astype(jnp.bfloat16)
            result = jnp.dot(vt_ref[h, :, :total], weight, preferred_element_type=jnp.float32)
            acc_ref[h] = acc_ref[h] * jnp.exp2(old - new) + result

        peaks = [scores(h) for h in range(LOOK)]
        for h in range(heads):
            if h + LOOK < heads:
                peaks.append(scores(h + LOOK))
            finish(h, peaks[h])

    ones = jnp.ones((heads, SUMS, vt_ref.shape[2]), jnp.bfloat16)
    vt_ref[:, HEAD_DIM:, :] = ones
    m_ref[...] = jnp.full(m_ref.shape, NEG, jnp.float32)
    acc_ref[...] = jnp.zeros(acc_ref.shape, jnp.float32)

    normed = slab_ref[OWN]
    loads[2].wait()
    wqt = wq_ref[...].T
    query = lax.dot_general(
        wqt, normed, (((1,), (1,)), ((), ())), preferred_element_type=jnp.float32
    ).astype(jnp.bfloat16).astype(jnp.float32) * SCALE
    high = query.astype(jnp.bfloat16)
    low = (query - high.astype(jnp.float32)).astype(jnp.bfloat16)
    zero = jnp.zeros((HEAD_DIM, rows), jnp.bfloat16)
    for h in range(heads):
        span = slice(h * HEAD_DIM, (h + 1) * HEAD_DIM)
        for part, base in ((high, 0), (low, PAIR)):
            here = base + (h % 2) * HEAD_DIM
            there = base + (1 - h % 2) * HEAD_DIM
            qt_ref[h, here:here + HEAD_DIM] = part[span]
            qt_ref[h, there:there + HEAD_DIM] = zero
    roll_call_early()
    loads[4].wait()
    wvt_ref[...] = wv_ref[...].T
    loads[3].wait()

    actions = {
        "p": lambda c: partner_copy().wait_recv(),
        "e": lambda c: roll_call_end(),
        "m": got_mirror, "r": got_rail,
        "c": got_cross,
    }

    def run(listed):
        for kind, low_c, high_c in listed:
            for c in range(low_c, high_c):
                actions[kind](c)

    def run_events(u, table):
        for k, listed in table.items():
            @pl.when(u == k)
            def _():
                run(listed)

    half = rows // 2

    def step(u, carry):
        run_events(u, {
            1: (("e", 0, 1), ("m", 0, 1)),
            2: (("p", 0, 1), ("m", 1, 2)),
            3: (("m", 2, 4),),
            4: (("m", 4, 5),),
            5: (("r", 0, 1), ("m", 5, 6), ("r", 1, 2), ("c", 0, 2)),
            6: (("m", 6, 7), ("r", 2, 4), ("m", 7, 8)),
            7: (("r", 4, 5), ("c", 2, 4)),
            8: (("r", 5, 6), ("c", 4, 6)),
            9: (("r", 6, 8), ("c", 6, 8)),
        })
        for k, listed in ((0, (0,)), (2, (1,)), (3, (2,)), (5, (3, 4))):
            @pl.when(u == k)
            def _():
                for i in listed:
                    masks[i].wait()
        plain = (u < 5) | (u == 6)
        slot = jnp.where(
            u < 3, u // 2,
            jnp.where(u == 4, PARTNER, jnp.where(plain, MIRROR, RAIL)),
        )
        start = jnp.where(
            u < 3, (u % 2) * half,
            jnp.where(
                plain, jnp.where(u == 3, 0, half),
                jnp.where(u == 5, 0, (u - 6) * PAIR),
            ),
        )
        slot_too = jnp.where(plain, slot, CROSS)
        start_too = jnp.where(plain, start + PAIR, start)
        unit([(slot, start), (slot_too, start_too)], PAIR)
        return carry

    lax.fori_loop(0, 5, step, 0)
    lax.fori_loop(5, 10, step, 0)

    for h in range(heads):
        inverse = 1.0 / acc_ref[h, HEAD_DIM:HEAD_DIM + 1]
        mixed_ref[h * HEAD_DIM:(h + 1) * HEAD_DIM, :] = (
            acc_ref[h, :HEAD_DIM] * inverse
        ).astype(jnp.bfloat16)
    for load in loads[5:]:
        load.wait()
    after_ref[...] = x_ref[...].astype(jnp.float32) + jnp.dot(
        mixed_ref[...].T, wo_ref[...], preferred_element_type=jnp.float32
    )

    local_mean = jnp.sum(after_ref[...], axis=0, keepdims=True) * (1.0 / rows)
    spread = after_ref[...] - local_mean
    stats_ref[0, 0:1] = local_mean
    stats_ref[0, 1:2] = jnp.sum(spread * spread, axis=0, keepdims=True)

    def stats_copy(source, target, device):
        return pltpu.make_async_remote_copy(
            src_ref=stats_ref.at[source], dst_ref=stats_ref.at[target],
            send_sem=s_send, recv_sem=s_recv,
            device_id={"blk": device}, device_id_type=MESH,
        )

    def send_stats(d, carry):
        e = jnp.where(2 * group < groups, n - d, d)
        stats_copy(0, e, lax.rem(me + e, n)).start()
        return carry

    lax.fori_loop(1, n, send_stats, 0)
    sent()
    others = pl.ds(1, n - 1)
    stats_copy(others, others, partner).wait_recv()
    gathered = stats_ref[...]
    means = gathered[:, 0, :]
    mean = jnp.sum(means, axis=0, keepdims=True) * (1.0 / n)
    shifts = means - mean
    var = (
        jnp.sum(gathered[:, 1, :], axis=0, keepdims=True) * (1.0 / rows)
        + jnp.sum(shifts * shifts, axis=0, keepdims=True)
    ) * (1.0 / n)
    gain = lax.rsqrt(var + 1e-05) * bg_ref[0:1]
    for piece in (slice(0, half), slice(half, rows)):
        batched = ((after_ref[piece] - mean) * gain + bs_ref[0:1]).astype(jnp.bfloat16)
        hidden = jax.nn.gelu(
            jnp.dot(batched, wu_ref[...], preferred_element_type=jnp.float32), approximate=True
        ).astype(jnp.bfloat16)
        out_ref[piece] = (
            after_ref[piece] + jnp.dot(hidden, wd_ref[...], preferred_element_type=jnp.float32)
        ).astype(jnp.bfloat16)

    stats_copy(others, others, partner).wait_send()


def body(
    atoms, edge_mask, norm_gain, w_query, w_key, w_value, w_out, bn_gain, bn_shift, w_up, w_down
):
    n = lax.axis_size("blk")
    rows, width = atoms.shape
    ff = w_up.shape[1]
    slabs = edge_mask.shape[1]
    heads = width // HEAD_DIM
    bf16, f32 = jnp.bfloat16, jnp.float32
    dma = pltpu.SemaphoreType.DMA
    return pl.pallas_call(
        functools.partial(kernel, n),
        out_shape=pltpu.VMEM((rows, width), bf16),
        in_specs=[pl.BlockSpec(memory_space=pl.ANY)] * 11,
        out_specs=pl.BlockSpec(memory_space=pltpu.VMEM),
        scratch_shapes=[
            pltpu.VMEM((rows, width), bf16),
            pltpu.VMEM((slabs, rows, width), bf16),
            pltpu.VMEM((slabs, rows, rows), jnp.int32),
            pltpu.VMEM((8, width), f32),
            pltpu.VMEM((width, width), bf16),
            pltpu.VMEM((width, width), bf16),
            pltpu.VMEM((width, width), bf16),
            pltpu.VMEM((width, width), bf16),
            pltpu.VMEM((8, width), f32),
            pltpu.VMEM((8, width), f32),
            pltpu.VMEM((width, ff), bf16),
            pltpu.VMEM((ff, width), bf16),
            pltpu.VMEM((width, width), bf16),
            pltpu.VMEM((heads, 2 * PAIR, rows), bf16),
            pltpu.VMEM((2 * PAIR, width), bf16),
            pltpu.VMEM((heads, HEAD_DIM + SUMS, 2 * PAIR), bf16),
            pltpu.VMEM((2 * PAIR, rows), f32),
            pltpu.VMEM((heads, 8, rows), f32),
            pltpu.VMEM((SLOTS, 2 * PAIR, rows), f32),
            pltpu.VMEM((heads, HEAD_DIM + SUMS, rows), f32),
            pltpu.VMEM((width, rows), bf16),
            pltpu.VMEM((rows, width), f32),
            pltpu.VMEM((n, 2, width), f32),
            dma((10,)),
            dma((slabs,)),
            dma, dma, dma, dma, dma,
            dma((3, CHUNKS)),
            dma, dma,
            pltpu.SemaphoreType.REGULAR, pltpu.SemaphoreType.REGULAR,
        ],
        compiler_params=pltpu.CompilerParams(
            collective_id=0, has_side_effects=True, vmem_limit_bytes=60 * 1024 * 1024
        ),
    )(
        atoms, edge_mask, norm_gain.reshape(1, width), w_query, w_key, w_value, w_out,
        bn_gain.reshape(1, width), bn_shift.reshape(1, width), w_up, w_down,
    )


def solution(mesh):
    placed = (
        P(("grp", "blk"), None),
        P(("grp", "blk"), None, None, None),
        P(), P(), P(), P(), P(), P(), P(), P(), P(),
    )
    return jax.shard_map(
        body, mesh=mesh, in_specs=placed, out_specs=P(("grp", "blk"), None), check_vma=False
    )
```
